256 devices in a mesh: row: 16 (over x, y), col: 16 (over z, core).
Axes of the slice: x: 4, y: 4, z: 8, core: 2. Of those that a mesh axis runs over, the one named last changes fastest.
Arguments:
- values: bfloat16 [8192, 8192], P('row', 'col'), may hold values from 0.0001296997 to 0.12988281
- tile_mask: int32 [64, 64], P('row', 'col'), may hold values 0 or 1
- keep_mask: int32 [64, 64], P('row', 'col'), may hold values 0 or 1
- thr_index: int32 [8192], P('col'), may hold values from 0 to 9
Outputs:
- expanded: bfloat16 [8192, 8192], P('row', 'col')
The draws below stay inside these ranges and needn't reach their ends.
All inputs are finite; a program needn't handle non-finite values. No bound on the sum of `tile_mask` or of `keep_mask` on one device may be relied on, other than what follows from the above.
Results may differ from the reference program's by a relative error of at most 0.0004.
Values may be sent and summed in bfloat16 or wider, within the bound.
A program may use at most 64 MiB of HBM per device.

```python
import math
import jax
import jax.numpy as jnp

TB = 128
NT = 64
ORDER = 8192


def touch_ends(values, stream_key, smallest, largest):
    spot = [jax.random.randint(jax.random.fold_in(stream_key, axis), (), 0, length) for axis, length in enumerate(values.shape)]
    longest = values.shape.index(max(values.shape))
    neighbour = spot[:longest] + [(spot[longest] + 1) % values.shape[longest]] + spot[longest + 1:]
    return values.at[tuple(spot)].set(smallest).at[tuple(neighbour)].set(largest)


def levels(stream_key, extent, shards, least, largest):
    level = 1.0
    for dim, shards_of in shards:
        draws = jax.random.uniform(jax.random.fold_in(jax.random.fold_in(stream_key, 6), dim), (shards_of,), jnp.float32, least / len(shards), largest / len(shards))
        level = level * jnp.repeat(jnp.exp(draws), extent[dim] // shards_of).reshape((-1,) + (1,) * (len(extent) - 1 - dim))
    return level


def setup_inputs(seed: int = 0) -> dict:
    seeds = jax.random.split(jax.random.key(seed), 5)
    values = jnp.clip(jnp.exp(math.log(0.12988281) - 6.909166 * jax.random.uniform(seeds[0], (ORDER, ORDER), jnp.float32) ** levels(seeds[0], (ORDER, ORDER), ((0, 16), (1, 16)), -0.2, 0.2)), 0.0001296997, 0.12988281).astype(jnp.bfloat16)
    tile_mask = touch_ends((jax.random.randint(seeds[1], (NT, NT), 0, 2) < 1).astype(jnp.int32), jax.random.fold_in(seeds[1], 1), 0, 1)
    keep_mask = touch_ends((jax.random.randint(seeds[2], (NT, NT), 0, 4) < 3).astype(jnp.int32), jax.random.fold_in(seeds[2], 1), 0, 1)
    thr_index = touch_ends(jax.random.randint(seeds[3], (ORDER,), 0, 10), jax.random.fold_in(seeds[3], 1), 0, 9).astype(jnp.int32)
    return {"values": values, "tile_mask": tile_mask, "keep_mask": keep_mask, "thr_index": thr_index}


def reference(values, tile_mask, keep_mask, thr_index):
    matrix = (values.reshape(NT, TB, NT, TB) * tile_mask[:, None, :, None].astype(jnp.bfloat16)).reshape(ORDER, ORDER)
    product = jnp.dot(matrix, matrix, preferred_element_type=jnp.float32)
    col_means = jnp.sum(product, axis=0) / ORDER
    thresholds = 0.125 * thr_index.astype(jnp.float32)
    kept_cells = jnp.broadcast_to(keep_mask[:, None, :, None].astype(jnp.float32), (NT, TB, NT, TB)).reshape(ORDER, ORDER)
    pruned = jnp.maximum(product - thresholds * col_means, 0.0) * kept_cells
    col_totals = jnp.sum(pruned, axis=0) / ORDER
    return (pruned / jnp.maximum(col_totals, 0.1)).astype(jnp.bfloat16)
```

```python
import jax
import jax.numpy as jnp
from jax import lax
from jax.experimental import pallas as pl
from jax.experimental.pallas import tpu as pltpu
from jax.sharding import PartitionSpec as P

TB = 128
BLK = 512
QR = 128
EXTRA = 16
NX = 4
NZ = 8
MESH = pl.DeviceIdType.MESH

XP = [(0, 0, 0), (0, 0, 1), (0, 0, 2), (0, 0, 3), (1, 0, 0), (1, 0, 2), (0, 1, 2), (0, 1, 3), (0, 3, 2), (0, 3, 3),
      (0, 2, 2), (0, 2, 3), (1, 1, 2), (1, 3, 2), (1, 2, 2)]
XM = [((-dx) % 4, (-dy) % 4, q ^ 1) for dx, dy, q in XP]
YP = [(dy, dx, q ^ 2) for dx, dy, q in XP]
YM = [(dy, dx, q ^ 2) for dx, dy, q in XM]
ZP = [(d, q) for d in range(3) for q in (0, 1, 2, 3)] + [(3, 0), (3, 1)]
ZM = [((-d) % 8, q ^ 2) for d, q in ZP]


def land(link, chunk):
    if link == "xp":
        return ((chunk[0] + 1) % 4, chunk[1], chunk[2])
    if link == "xm":
        return ((chunk[0] - 1) % 4, chunk[1], chunk[2])
    if link == "yp":
        return (chunk[0], (chunk[1] + 1) % 4, chunk[2])
    if link == "ym":
        return (chunk[0], (chunk[1] - 1) % 4, chunk[2])
    if link == "zp":
        return ((chunk[0] + 1) % 8, chunk[1])
    return ((chunk[0] - 1) % 8, chunk[1])


LINKS = {"xp": XP, "xm": XM, "yp": YP, "ym": YM, "zp": ZP, "zm": ZM}
ROUND_B = {(0, 0): -1}
for _link in ("xp", "xm", "yp", "ym"):
    for _r, _c in enumerate(LINKS[_link]):
        _l = land(_link, _c)
        ROUND_B[_l[:2]] = max(ROUND_B.get(_l[:2], -1), _r)
LAST = len(XP) - 1


def kernel(values_ref, tile_ref, keep_ref, thr_ref, out_ref, raw, abuf, bbuf, acc, own, pbuf, sbuf, tbuf,
           raw_sem, send_xy, send_z, send_d, send_small, recv_b, recv_a, recv_d, recv_p, recv_s, recv_t, ready):
    row, col = lax.axis_index("row"), lax.axis_index("col")
    x, y, z, core = row // 4, row % 4, col // 2, col % 2

    def at(dx, dy):
        return (((x + dx + 4) % 4) * 4 + (y + dy + 4) % 4, col)

    def along(dz, other):
        return (row, ((z + dz + 8) % 8) * 2 + (core + other) % 2)

    peer = {"xp": at(1, 0), "xm": at(-1, 0), "yp": at(0, 1), "ym": at(0, -1), "zp": along(1, 0), "zm": along(-1, 0)}
    partner = along(0, 1)
    neighbours = list(peer.values()) + [partner]

    barrier = pltpu.get_barrier_semaphore()
    for n in neighbours:
        pl.semaphore_signal(barrier, inc=1, device_id=n, device_id_type=MESH)
    fetch = pltpu.make_async_copy(values_ref, raw, raw_sem)
    fetch.start()
    acc[...] = jnp.zeros_like(acc)
    fetch.wait()
    sums = [jnp.zeros((1, TB), jnp.float32) for _ in range(4)]
    for i in range(4):
        for j in range(4):
            tile = raw[pl.ds(i * TB, TB), pl.ds(j * TB, TB)].astype(jnp.float32) * tile_ref[i, j].astype(jnp.float32)
            sums[j] = sums[j] + jnp.sum(tile, axis=0, keepdims=True)
            tile = tile.astype(jnp.bfloat16)
            abuf[0, pl.ds(i * TB, TB), pl.ds(j * TB, TB)] = tile
            bbuf[0, pl.ds(i * TB, TB), pl.ds(j * TB, TB)] = tile
    for j in range(4):
        pbuf[0, :, pl.ds(j * TB, TB)] = sums[j]
    pl.semaphore_wait(barrier, len(neighbours))

    def quarter(buf, slot, q):
        return buf.at[slot, pl.ds(q * QR, QR), :]

    have = {("b", 0, 0, q) for q in range(4)} | {("a", 0, q) for q in range(4)}
    nxt = dict.fromkeys(LINKS, 0)
    sent = {"xy": [], "z": [], "d": [], "small": []}

    def advance():
        more = True
        while more:
            more = False
            for link, chunks in LINKS.items():
                if nxt[link] == len(chunks):
                    continue
                c = chunks[nxt[link]]
                kind = "a" if link[0] == "z" else "b"
                if (kind,) + c not in have:
                    continue
                to = land(link, c)
                if kind == "b":
                    src, dst = quarter(bbuf, c[0] * 4 + c[1], c[2]), quarter(bbuf, to[0] * 4 + to[1], to[2])
                    ss, rs = send_xy.at[len(sent["xy"])], recv_b.at[to[0] * 4 + to[1], to[2]]
                else:
                    src, dst = quarter(abuf, c[0] * 2, c[1]), quarter(abuf, to[0] * 2, to[1])
                    ss, rs = send_z.at[len(sent["z"])], recv_a.at[to[0], to[1]]
                copy = pltpu.make_async_remote_copy(src, dst, ss, rs, device_id=peer[link], device_id_type=MESH)
                copy.start()
                sent["xy" if kind == "b" else "z"].append(copy)
                nxt[link] += 1
                more = True

    def half(slot, h):
        return abuf.at[slot, pl.ds(h * 256, 256), :]

    def hand_over(dz, h):
        copy = pltpu.make_async_remote_copy(half(dz * 2, h), half(dz * 2 + 1, h), send_d.at[len(sent["d"])],
                                            recv_d.at[dz, h], device_id=partner, device_id_type=MESH)
        copy.start()
        sent["d"].append(copy)

    def take_over(dz):
        for h in range(2):
            pltpu.make_async_remote_copy(half(dz * 2, h), half(dz * 2 + 1, h), send_d.at[0], recv_d.at[dz, h],
                                         device_id=partner, device_id_type=MESH).wait_recv()

    handed = set()

    def arrive(r):
        for link, chunks in LINKS.items():
            if r >= len(chunks):
                continue
            to = land(link, chunks[r])
            if link[0] == "z":
                ref = quarter(abuf, to[0] * 2, to[1])
                sem = recv_a.at[to[0], to[1]]
                have.add(("a",) + to)
            else:
                ref = quarter(bbuf, to[0] * 4 + to[1], to[2])
                sem = recv_b.at[to[0] * 4 + to[1], to[2]]
                have.add(("b",) + to)
            pltpu.make_async_remote_copy(ref, ref, send_d.at[0], sem, device_id=partner,
                                         device_id_type=MESH).wait_recv()
            advance()
            if link[0] == "z":
                for h in range(2):
                    if (to[0], h) not in handed and all(("a", to[0], 2 * h + k) in have for k in range(2)):
                        handed.add((to[0], h))
                        hand_over(to[0], h)

    def greet(i):
        for n in neighbours:
            pl.semaphore_signal(ready.at[i], inc=1, device_id=n, device_id_type=MESH)
        pl.semaphore_wait(ready.at[i], len(neighbours))

    def small(src, dst, sem, to):
        copy = pltpu.make_async_remote_copy(src, dst, send_small.at[len(sent["small"])], sem, device_id=to,
                                            device_id_type=MESH)
        copy.start()
        sent["small"].append(copy)

    def small_wait(ref, sem):
        pltpu.make_async_remote_copy(ref, ref, send_d.at[0], sem, device_id=partner, device_id_type=MESH).wait_recv()

    def left_slot(i):
        origin = ((x - i // 4 + 4) % 4) * 4 + (y - i % 4 + 4) % 4
        dz = (z - origin // 2 + 8) % 8
        return dz, (origin % 2 + core) % 2

    def multiply(i):
        dz, other = left_slot(i)
        acc[...] += jnp.dot(abuf[dz * 2 + other], bbuf[i], preferred_element_type=jnp.float32)

    def round_of(i):
        dz, other = left_slot(i)
        far = jnp.minimum(dz, 8 - dz)
        ra = jnp.minimum(4 * far - 1, 13) + other
        rb = jnp.int32(-1)
        for (dx, dy), r in ROUND_B.items():
            rb = jnp.where(i == dx * 4 + dy, jnp.int32(r), rb)
        return jnp.maximum(ra, rb)

    def multiply_ready(lo, hi):
        def step(i, carry):
            r = round_of(i)

            @pl.when((r >= lo) & (r < hi))
            def _():
                multiply(i)

            return carry

        lax.fori_loop(0, 16, step, 0)

    advance()
    for h in range(2):
        handed.add((0, h))
        hand_over(0, h)
    for i in range(3):
        greet(i)
    for a in range(4):
        for b in range(4):
            if (a, b) != (0, 0):
                small(pbuf.at[0], pbuf.at[a * 4 + b], recv_p.at[a * 4 + b], at(a, b))
    greet(3)
    arrive(0)
    for s in range(1, 16):
        small_wait(pbuf.at[s], recv_p.at[s])
    own_s = pbuf[0]
    for s in range(1, 16):
        own_s = own_s + pbuf[s]
    sbuf[0] = own_s
    arrive(1)
    for d in range(8):
        for other in range(2):
            if (d, other) != (0, 0):
                small(sbuf.at[0], sbuf.at[d * 2 + other], recv_s.at[d * 2 + other], along(d, other))
    arrive(2)
    arrive(3)
    for s in range(1, 16):
        small_wait(sbuf.at[s], recv_s.at[s])
    for s in range(16):
        v = sbuf[s]
        p0 = v.astype(jnp.bfloat16).astype(jnp.float32)
        p1 = (v - p0).astype(jnp.bfloat16).astype(jnp.float32)
        p2 = v - p0 - p1
        rows = lax.broadcasted_iota(jnp.int32, (EXTRA, BLK), 0)
        block = jnp.where(rows == 0, p0, jnp.where(rows == 1, p1, jnp.where(rows == 2, p2, 0.0)))
        abuf[s, pl.ds(BLK, EXTRA), :] = block.astype(jnp.bfloat16)
    take_over(0)
    multiply_ready(-2, 4)
    done = 4
    for r in range(4, 14):
        arrive(r)
        if r == 4:
            take_over(1)
            take_over(7)
        if r == 8:
            take_over(2)
            take_over(6)
        if r == 12:
            take_over(3)
            take_over(5)
        if r in (5, 7, 9, 11, 12, 13):
            multiply_ready(done, r + 1)
            done = r + 1
    take_over(4)
    far = ((z + 4) % 8) * 2 + (core + 1) % 2
    far_slot = ((x - far // 4 + 4) % 4) * 4 + (y - far % 4 + 4) % 4

    @pl.when(far_slot != 10)
    def _():
        multiply(far_slot)

    arrive(14)
    multiply(10)

    col_means = (acc[BLK : BLK + 1] + acc[BLK + 1 : BLK + 2] + acc[BLK + 2 : BLK + 3]) / (BLK * 16)
    cut = 0.125 * thr_ref[...].astype(jnp.float32) * col_means
    for j in range(4):
        total = jnp.zeros((1, TB), jnp.float32)
        for i in range(4):
            part = acc[pl.ds(i * TB, TB), pl.ds(j * TB, TB)]
            part = jnp.maximum(part - cut[:, j * TB : (j + 1) * TB], 0.0) * keep_ref[i, j].astype(jnp.float32)
            acc[pl.ds(i * TB, TB), pl.ds(j * TB, TB)] = part
            total = total + jnp.sum(part, axis=0, keepdims=True)
        tbuf[0, :, pl.ds(j * TB, TB)] = total
    for a in range(4):
        for b in range(4):
            if (a, b) != (0, 0):
                small(tbuf.at[0], tbuf.at[a * 4 + b], recv_t.at[a * 4 + b], at(a, b))
    for group in sent.values():
        for copy in group:
            copy.wait_send()
    total = tbuf[0]
    for s in range(1, 16):
        small_wait(tbuf.at[s], recv_t.at[s])
        total = total + tbuf[s]
    scale = jnp.maximum(total / (BLK * 16), 0.1)
    out_ref[...] = (acc[:BLK] / scale).astype(jnp.bfloat16)


def on_device(values, tile_mask, keep_mask, thr_index):
    dma = pltpu.SemaphoreType.DMA
    return pl.pallas_call(
        kernel,
        out_shape=jax.ShapeDtypeStruct(values.shape, jnp.bfloat16),
        in_specs=[
            pl.BlockSpec(memory_space=pl.ANY),
            pl.BlockSpec(memory_space=pltpu.SMEM),
            pl.BlockSpec(memory_space=pltpu.SMEM),
            pl.BlockSpec(memory_space=pltpu.VMEM),
        ],
        out_specs=pl.BlockSpec(memory_space=pltpu.VMEM),
        scratch_shapes=[
            pltpu.VMEM((BLK, BLK), jnp.bfloat16),
            pltpu.VMEM((16, BLK + EXTRA, BLK), jnp.bfloat16),
            pltpu.VMEM((16, BLK, BLK), jnp.bfloat16),
            pltpu.VMEM((BLK + EXTRA, BLK), jnp.float32),
            pltpu.VMEM((1, BLK), jnp.float32),
            pltpu.VMEM((16, 1, BLK), jnp.float32),
            pltpu.VMEM((16, 1, BLK), jnp.float32),
            pltpu.VMEM((16, 1, BLK), jnp.float32),
            dma,
            dma((60,)),
            dma((28,)),
            dma((16,)),
            dma((45,)),
            dma((16, 4)),
            dma((8, 4)),
            dma((8, 2)),
            dma((16,)),
            dma((16,)),
            dma((16,)),
            pltpu.SemaphoreType.REGULAR((4,)),
        ],
        compiler_params=pltpu.CompilerParams(collective_id=0, has_side_effects=True, vmem_limit_bytes=48 << 20),
    )(values, tile_mask, keep_mask, thr_index.reshape(1, BLK))


def solution(mesh):
    placed = (P("row", "col"), P("row", "col"), P("row", "col"), P("col"))
    return jax.shard_map(on_device, mesh=mesh, in_specs=placed, out_specs=P("row", "col"), check_vma=False)
```

```python
import jax
import jax.numpy as jnp
from jax import lax
from jax.experimental import pallas as pl
from jax.experimental.pallas import tpu as pltpu
from jax.sharding import PartitionSpec as P

TB = 128
BLK = 512
QR = 128
EXTRA = 16
NX = 4
NZ = 8
MESH = pl.DeviceIdType.MESH

XP = [(0, 0, 0), (0, 0, 1), (0, 0, 2), (0, 0, 3), (1, 0, 0), (1, 0, 2), (0, 1, 2), (0, 1, 3), (0, 3, 2), (0, 3, 3),
      (0, 2, 2), (0, 2, 3), (1, 1, 2), (1, 3, 2), (1, 2, 2)]
XM = [((-dx) % 4, (-dy) % 4, q ^ 1) for dx, dy, q in XP]
YP = [(dy, dx, q ^ 2) for dx, dy, q in XP]
YM = [(dy, dx, q ^ 2) for dx, dy, q in XM]
ZP = [(d, q) for d in range(3) for q in (0, 1, 2, 3)] + [(3, 0), (3, 1)]
ZM = [((-d) % 8, q ^ 2) for d, q in ZP]


def land(link, chunk):
    if link == "xp":
        return ((chunk[0] + 1) % 4, chunk[1], chunk[2])
    if link == "xm":
        return ((chunk[0] - 1) % 4, chunk[1], chunk[2])
    if link == "yp":
        return (chunk[0], (chunk[1] + 1) % 4, chunk[2])
    if link == "ym":
        return (chunk[0], (chunk[1] - 1) % 4, chunk[2])
    if link == "zp":
        return ((chunk[0] + 1) % 8, chunk[1])
    return ((chunk[0] - 1) % 8, chunk[1])


LINKS = {"xp": XP, "xm": XM, "yp": YP, "ym": YM, "zp": ZP, "zm": ZM}
ROUND_B = {(0, 0): -1}
for _link in ("xp", "xm", "yp", "ym"):
    for _r, _c in enumerate(LINKS[_link]):
        _l = land(_link, _c)
        ROUND_B[_l[:2]] = max(ROUND_B.get(_l[:2], -1), _r)
LAST = len(XP) - 1


def kernel(values_ref, tile_hbm, keep_hbm, thr_hbm, out_ref, raw, tile_ref, keep_ref, thr_ref, abuf, bbuf, acc, own, pbuf, sbuf, tbuf,
           raw_sem, send_xy, send_z, send_d, send_small, recv_b, recv_a, recv_d, recv_p, recv_s, recv_t, ready):
    row, col = lax.axis_index("row"), lax.axis_index("col")
    x, y, z, core = row // 4, row % 4, col // 2, col % 2

    def at(dx, dy):
        return (((x + dx + 4) % 4) * 4 + (y + dy + 4) % 4, col)

    def along(dz, other):
        return (row, ((z + dz + 8) % 8) * 2 + (core + other) % 2)

    peer = {"xp": at(1, 0), "xm": at(-1, 0), "yp": at(0, 1), "ym": at(0, -1), "zp": along(1, 0), "zm": along(-1, 0)}
    partner = along(0, 1)
    neighbours = list(peer.values()) + [partner]

    barrier = pltpu.get_barrier_semaphore()
    for n in neighbours:
        pl.semaphore_signal(barrier, inc=1, device_id=n, device_id_type=MESH)
    fetches = [
        pltpu.make_async_copy(src, dst, raw_sem.at[i])
        for i, (src, dst) in enumerate(
            [(tile_hbm, tile_ref), (values_ref, raw), (keep_hbm, keep_ref), (thr_hbm, thr_ref)]
        )
    ]
    for fetch in fetches:
        fetch.start()
    acc[...] = jnp.zeros_like(acc)
    for fetch in fetches:
        fetch.wait()
    sums = [jnp.zeros((1, TB), jnp.float32) for _ in range(4)]
    for i in range(4):
        for j in range(4):
            tile = raw[pl.ds(i * TB, TB), pl.ds(j * TB, TB)].astype(jnp.float32) * tile_ref[i, j].astype(jnp.float32)
            sums[j] = sums[j] + jnp.sum(tile, axis=0, keepdims=True)
            tile = tile.astype(jnp.bfloat16)
            abuf[0, pl.ds(i * TB, TB), pl.ds(j * TB, TB)] = tile
            bbuf[0, pl.ds(i * TB, TB), pl.ds(j * TB, TB)] = tile
    for j in range(4):
        pbuf[0, :, pl.ds(j * TB, TB)] = sums[j]
    pl.semaphore_wait(barrier, len(neighbours))

    def quarter(buf, slot, q):
        return buf.at[slot, pl.ds(q * QR, QR), :]

    have = {("b", 0, 0, q) for q in range(4)} | {("a", 0, q) for q in range(4)}
    nxt = dict.fromkeys(LINKS, 0)
    sent = {"xy": [], "z": [], "d": [], "small": []}

    def advance():
        more = True
        while more:
            more = False
            for link, chunks in LINKS.items():
                if nxt[link] == len(chunks):
                    continue
                c = chunks[nxt[link]]
                kind = "a" if link[0] == "z" else "b"
                if (kind,) + c not in have:
                    continue
                to = land(link, c)
                if kind == "b":
                    src, dst = quarter(bbuf, c[0] * 4 + c[1], c[2]), quarter(bbuf, to[0] * 4 + to[1], to[2])
                    ss, rs = send_xy.at[len(sent["xy"])], recv_b.at[to[0] * 4 + to[1], to[2]]
                else:
                    src, dst = quarter(abuf, c[0] * 2, c[1]), quarter(abuf, to[0] * 2, to[1])
                    ss, rs = send_z.at[len(sent["z"])], recv_a.at[to[0], to[1]]
                copy = pltpu.make_async_remote_copy(src, dst, ss, rs, device_id=peer[link], device_id_type=MESH)
                copy.start()
                sent["xy" if kind == "b" else "z"].append(copy)
                nxt[link] += 1
                more = True

    def half(slot, h):
        return abuf.at[slot, pl.ds(h * 256, 256), :]

    def hand_over(dz, h):
        copy = pltpu.make_async_remote_copy(half(dz * 2, h), half(dz * 2 + 1, h), send_d.at[len(sent["d"])],
                                            recv_d.at[dz, h], device_id=partner, device_id_type=MESH)
        copy.start()
        sent["d"].append(copy)

    def take_over(dz):
        for h in range(2):
            pltpu.make_async_remote_copy(half(dz * 2, h), half(dz * 2 + 1, h), send_d.at[0], recv_d.at[dz, h],
                                         device_id=partner, device_id_type=MESH).wait_recv()

    handed = set()

    def arrive(r):
        for link, chunks in LINKS.items():
            if r >= len(chunks):
                continue
            to = land(link, chunks[r])
            if link[0] == "z":
                ref = quarter(abuf, to[0] * 2, to[1])
                sem = recv_a.at[to[0], to[1]]
                have.add(("a",) + to)
            else:
                ref = quarter(bbuf, to[0] * 4 + to[1], to[2])
                sem = recv_b.at[to[0] * 4 + to[1], to[2]]
                have.add(("b",) + to)
            pltpu.make_async_remote_copy(ref, ref, send_d.at[0], sem, device_id=partner,
                                         device_id_type=MESH).wait_recv()
            advance()
            if link[0] == "z":
                for h in range(2):
                    if (to[0], h) not in handed and all(("a", to[0], 2 * h + k) in have for k in range(2)):
                        handed.add((to[0], h))
                        hand_over(to[0], h)

    def greet(i):
        for n in neighbours:
            pl.semaphore_signal(ready.at[i], inc=1, device_id=n, device_id_type=MESH)
        pl.semaphore_wait(ready.at[i], len(neighbours))

    def small(src, dst, sem, to):
        copy = pltpu.make_async_remote_copy(src, dst, send_small.at[len(sent["small"])], sem, device_id=to,
                                            device_id_type=MESH)
        copy.start()
        sent["small"].append(copy)

    def small_wait(ref, sem):
        pltpu.make_async_remote_copy(ref, ref, send_d.at[0], sem, device_id=partner, device_id_type=MESH).wait_recv()

    def left_slot(i):
        origin = ((x - i // 4 + 4) % 4) * 4 + (y - i % 4 + 4) % 4
        dz = (z - origin // 2 + 8) % 8
        return dz, (origin % 2 + core) % 2

    def multiply(i):
        dz, other = left_slot(i)
        acc[...] += jnp.dot(abuf[dz * 2 + other], bbuf[i], preferred_element_type=jnp.float32)

    def round_of(i):
        dz, other = left_slot(i)
        far = jnp.minimum(dz, 8 - dz)
        ra = jnp.minimum(4 * far - 1, 13) + other
        rb = jnp.int32(-1)
        for (dx, dy), r in ROUND_B.items():
            rb = jnp.where(i == dx * 4 + dy, jnp.int32(r), rb)
        return jnp.maximum(ra, rb)

    def multiply_ready(lo, hi):
        def step(i, carry):
            r = round_of(i)

            @pl.when((r >= lo) & (r < hi))
            def _():
                multiply(i)

            return carry

        lax.fori_loop(0, 16, step, 0)

    advance()
    for h in range(2):
        handed.add((0, h))
        hand_over(0, h)
    for i in range(3):
        greet(i)
    for a in range(4):
        for b in range(4):
            if (a, b) != (0, 0):
                small(pbuf.at[0], pbuf.at[a * 4 + b], recv_p.at[a * 4 + b], at(a, b))
    greet(3)
    arrive(0)
    for s in range(1, 16):
        small_wait(pbuf.at[s], recv_p.at[s])
    own_s = pbuf[0]
    for s in range(1, 16):
        own_s = own_s + pbuf[s]
    sbuf[0] = own_s
    arrive(1)
    for d in range(8):
        for other in range(2):
            if (d, other) != (0, 0):
                small(sbuf.at[0], sbuf.at[d * 2 + other], recv_s.at[d * 2 + other], along(d, other))
    arrive(2)
    arrive(3)
    for s in range(1, 16):
        small_wait(sbuf.at[s], recv_s.at[s])
    for s in range(16):
        v = sbuf[s]
        p0 = v.astype(jnp.bfloat16).astype(jnp.float32)
        p1 = (v - p0).astype(jnp.bfloat16).astype(jnp.float32)
        p2 = v - p0 - p1
        rows = lax.broadcasted_iota(jnp.int32, (EXTRA, BLK), 0)
        block = jnp.where(rows == 0, p0, jnp.where(rows == 1, p1, jnp.where(rows == 2, p2, 0.0)))
        abuf[s, pl.ds(BLK, EXTRA), :] = block.astype(jnp.bfloat16)
    take_over(0)
    multiply_ready(-2, 4)
    done = 4
    for r in range(4, 14):
        arrive(r)
        if r == 4:
            take_over(1)
            take_over(7)
        if r == 8:
            take_over(2)
            take_over(6)
        if r == 12:
            take_over(3)
            take_over(5)
        if r in (5, 7, 9, 11, 12, 13):
            multiply_ready(done, r + 1)
            done = r + 1
    take_over(4)
    far = ((z + 4) % 8) * 2 + (core + 1) % 2
    far_slot = ((x - far // 4 + 4) % 4) * 4 + (y - far % 4 + 4) % 4

    @pl.when(far_slot != 10)
    def _():
        multiply(far_slot)

    arrive(14)
    multiply(10)

    col_means = (acc[BLK : BLK + 1] + acc[BLK + 1 : BLK + 2] + acc[BLK + 2 : BLK + 3]) / (BLK * 16)
    cut = 0.125 * thr_ref[...].astype(jnp.float32) * col_means
    for j in range(4):
        total = jnp.zeros((1, TB), jnp.float32)
        for i in range(4):
            part = acc[pl.ds(i * TB, TB), pl.ds(j * TB, TB)]
            part = jnp.maximum(part - cut[:, j * TB : (j + 1) * TB], 0.0) * keep_ref[i, j].astype(jnp.float32)
            acc[pl.ds(i * TB, TB), pl.ds(j * TB, TB)] = part
            total = total + jnp.sum(part, axis=0, keepdims=True)
        tbuf[0, :, pl.ds(j * TB, TB)] = total
    for a in range(4):
        for b in range(4):
            if (a, b) != (0, 0):
                small(tbuf.at[0], tbuf.at[a * 4 + b], recv_t.at[a * 4 + b], at(a, b))
    for group in sent.values():
        for copy in group:
            copy.wait_send()
    total = tbuf[0]
    for s in range(1, 16):
        small_wait(tbuf.at[s], recv_t.at[s])
        total = total + tbuf[s]
    scale = jnp.maximum(total / (BLK * 16), 0.1)
    out_ref[...] = (acc[:BLK] / scale).astype(jnp.bfloat16)


def on_device(values, tile_mask, keep_mask, thr_index):
    dma = pltpu.SemaphoreType.DMA
    return pl.pallas_call(
        kernel,
        out_shape=jax.ShapeDtypeStruct(values.shape, jnp.bfloat16),
        in_specs=[pl.BlockSpec(memory_space=pltpu.HBM)] * 4,
        out_specs=pl.BlockSpec(memory_space=pltpu.VMEM),
        scratch_shapes=[
            pltpu.VMEM((BLK, BLK), jnp.bfloat16),
            pltpu.SMEM((4, 4), jnp.int32),
            pltpu.SMEM((4, 4), jnp.int32),
            pltpu.VMEM((1, BLK), jnp.int32),
            pltpu.VMEM((16, BLK + EXTRA, BLK), jnp.bfloat16),
            pltpu.VMEM((16, BLK, BLK), jnp.bfloat16),
            pltpu.VMEM((BLK + EXTRA, BLK), jnp.float32),
            pltpu.VMEM((1, BLK), jnp.float32),
            pltpu.VMEM((16, 1, BLK), jnp.float32),
            pltpu.VMEM((16, 1, BLK), jnp.float32),
            pltpu.VMEM((16, 1, BLK), jnp.float32),
            dma((4,)),
            dma((60,)),
            dma((28,)),
            dma((16,)),
            dma((45,)),
            dma((16, 4)),
            dma((8, 4)),
            dma((8, 2)),
            dma((16,)),
            dma((16,)),
            dma((16,)),
            pltpu.SemaphoreType.REGULAR((4,)),
        ],
        compiler_params=pltpu.CompilerParams(collective_id=0, has_side_effects=True, vmem_limit_bytes=48 << 20),
    )(*[pltpu.with_memory_space_constraint(v, pltpu.HBM) for v in (values, tile_mask, keep_mask, thr_index.reshape(1, BLK))])


def solution(mesh):
    placed = (P("row", "col"), P("row", "col"), P("row", "col"), P("col"))
    return jax.shard_map(on_device, mesh=mesh, in_specs=placed, out_specs=P("row", "col"), check_vma=False)
```

```python
import jax
import jax.numpy as jnp
from jax import lax
from jax.experimental import pallas as pl
from jax.experimental.pallas import tpu as pltpu
from jax.sharding import PartitionSpec as P

TB = 128
BLK = 512
QR = 128
NX = 4
NZ = 8
MESH = pl.DeviceIdType.MESH

OWN = [(0, 0, 0), (0, 0, 1), (0, 0, 2), (0, 0, 3)]
XP = OWN + [(1, 0, 0), (1, 0, 2), (0, 1, 2), (0, 1, 3), (0, 3, 2), (0, 3, 3), (0, 2, 2), (0, 2, 3), (1, 1, 2), (1, 3, 2),
            (1, 2, 2)]
XM = OWN + [((-dx) % 4, dy, q ^ 1) for dx, dy, q in XP[4:]]
YP = OWN + [(dy, dx, q ^ 2) for dx, dy, q in [XP[5], XP[4]] + XP[6:]]
YM = OWN + [(dy, dx, q ^ 2) for dx, dy, q in [XM[5], XM[4]] + XM[6:]]
ZP = [(d, q) for d in (0, 1, 2) for q in range(4)] + [(3, 0), (3, 1)]
ZM = [(d, q) for d in (0, 7, 6) for q in range(4)] + [(5, 2), (5, 3)]
LINKS = {"xp": XP, "xm": XM, "yp": YP, "ym": YM, "zp": ZP, "zm": ZM}
STEP = {"xp": (1, 0, 0), "xm": (3, 0, 0), "yp": (0, 1, 0), "ym": (0, 3, 0), "zp": (1, 0), "zm": (7, 0)}


def land(link, chunk):
    extent = 8 if link[0] == "z" else 4
    moved = [(a + b) % extent for a, b in zip(chunk, STEP[link])]
    return tuple(moved[:-1]) + (chunk[-1],)


EVENT_OF_ROUND = [0, 0, 0, 0, 1, 1, 2, 2, 3, 3, 4, 4, 5, 6, 7]
EVENT_B = [0] * 16
for _link in ("xp", "xm", "yp", "ym"):
    for _r, _c in enumerate(LINKS[_link]):
        _l = land(_link, _c)
        EVENT_B[_l[0] * 4 + _l[1]] = max(EVENT_B[_l[0] * 4 + _l[1]], EVENT_OF_ROUND[_r])
EVENT_A = [0, 0, 1, 2, 3, 4, 6, 7, 8, 9, 5, 7, 3, 4, 1, 2]


def kernel(values_ref, tile_hbm, keep_hbm, thr_hbm, out_ref, raw, tile_ref, keep_ref, thr_ref, abuf, bbuf, acc, pbuf, sbuf,
           vbuf, tbuf, raw_sem, send_xy, send_z, send_d, send_p, send_s, send_v, send_t, recv_b, recv_a, recv_d, recv_p,
           recv_s, recv_v, recv_t, go, ready):
    row, col = lax.axis_index("row"), lax.axis_index("col")
    x, y, z, core = row // 4, row % 4, col // 2, col % 2

    def at(dx, dy):
        return (((x + dx + 4) % 4) * 4 + (y + dy + 4) % 4, col)

    def along(dz, other):
        return (row, ((z + dz + 8) % 8) * 2 + (core + other) % 2)

    def signal(sem, to):
        pl.semaphore_signal(sem, inc=1, device_id=to, device_id_type=MESH)

    peer = {"xp": at(1, 0), "xm": at(-1, 0), "yp": at(0, 1), "ym": at(0, -1), "zp": along(1, 0), "zm": along(-1, 0)}
    partner = along(0, 1)
    plane = [peer[link] for link in ("xp", "xm", "yp", "ym")]
    line = [peer["zp"], peer["zm"]]
    late_p = (z % 4) // 3
    late_m = (3 - z % 4) // 3
    late = late_p + late_m

    barrier = pltpu.get_barrier_semaphore()
    for to in plane:
        signal(barrier, (to[0], z * 2))
    signal(barrier, (row, ((z + 1) % 8) * 2 + late_p))
    signal(barrier, (row, ((z + 7) % 8) * 2 + late_m))

    @pl.when(core == 1)
    def _():
        signal(barrier, partner)

    tiles = pltpu.make_async_copy(tile_hbm, tile_ref, raw_sem.at[0])
    tiles.start()
    fetches = [
        pltpu.make_async_copy(
            values_ref.at[pl.ds(i * QR, QR), :], raw.at[pl.ds(i * QR, QR), :], raw_sem.at[1 + i]
        )
        for i in range(4)
    ]
    for fetch in fetches:
        fetch.start()
    rest = [
        pltpu.make_async_copy(keep_hbm, keep_ref, raw_sem.at[5]),
        pltpu.make_async_copy(thr_hbm, thr_ref, raw_sem.at[6]),
    ]
    for fetch in rest:
        fetch.start()

    def mask(i):
        fetches[i].wait()
        for j in range(4):
            tile = raw[pl.ds(i * TB, TB), pl.ds(j * TB, TB)].astype(jnp.float32) * tile_ref[i, j].astype(jnp.float32)
            tile = tile.astype(jnp.bfloat16)
            abuf[0, pl.ds(i * TB, TB), pl.ds(j * TB, TB)] = tile
            bbuf[0, pl.ds(i * TB, TB), pl.ds(j * TB, TB)] = tile

    sent = []

    def remote(src, dst, ss, rs, to):
        return pltpu.make_async_remote_copy(src, dst, ss, rs, device_id=to, device_id_type=MESH)

    def arrived(ref, sem):
        remote(ref, ref, send_d.at[0], sem, partner).wait_recv()

    def quarter(buf, slot, q):
        return buf.at[slot, pl.ds(q * QR, QR), :]

    def half(slot, h):
        return abuf.at[slot, pl.ds(h * 256, 256), :]

    have = set()
    nxt = dict.fromkeys(("xp", "xm", "yp", "ym"), 0)
    n_xy = [0]

    def advance():
        more = True
        while more:
            more = False
            for link in nxt:
                if nxt[link] == len(LINKS[link]) or LINKS[link][nxt[link]] not in have:
                    continue
                c = LINKS[link][nxt[link]]
                to = land(link, c)
                copy = remote(
                    quarter(bbuf, c[0] * 4 + c[1], c[2]),
                    quarter(bbuf, to[0] * 4 + to[1], to[2]),
                    send_xy.at[n_xy[0]],
                    recv_b.at[to[0] * 4 + to[1], to[2]],
                    peer[link],
                )
                copy.start()
                sent.append(copy)
                n_xy[0] += 1
                nxt[link] += 1
                more = True

    def along_xy(r):
        for link in nxt:
            to = land(link, LINKS[link][r])
            arrived(quarter(bbuf, to[0] * 4 + to[1], to[2]), recv_b.at[to[0] * 4 + to[1], to[2]])
            have.add(to)
            advance()

    def z_copy(link, c, slot):
        to = land(link, c)
        return remote(
            quarter(abuf, c[0] * 2, c[1]), quarter(abuf, to[0] * 2, to[1]), send_z.at[slot], recv_a.at[to[0], to[1]], peer[link]
        )

    def send_along_z(link, r):
        z_copy(link, LINKS[link][r], r if link == "zp" else 14 + r).start()

    def hand_over(dz, h):
        copy = remote(half(dz * 2, h), half(dz * 2 + 1, h), send_d.at[dz * 2 + h], recv_d.at[dz, h], partner)
        copy.start()
        sent.append(copy)

    def take_over(dz):
        for h in range(2):
            arrived(half(dz * 2 + 1, h), recv_d.at[dz, h])

    def along_z(link, r):
        to = land(link, LINKS[link][r])
        arrived(quarter(abuf, to[0] * 2, to[1]), recv_a.at[to[0], to[1]])
        if to in LINKS[link]:
            n = LINKS[link].index(to)
            if link == "zp" and n == 13:
                @pl.when(z != 7)
                def _():
                    send_along_z(link, n)

            else:
                send_along_z(link, n)
        elif link == "zm" and to == (5, 1):

            @pl.when(z == 1)
            def _():
                z_copy(link, to, 28).start()

        if r % 2 == 1:
            hand_over(to[0], to[1] // 2)

    def own_along_z(q):
        @pl.when(late_p == 0)
        def _():
            send_along_z("zp", q)

        @pl.when(late_m == 0)
        def _():
            send_along_z("zm", q)

    def across(when):
        @pl.when(when & (late > 0))
        def _():
            @pl.when(core == 1)
            def _():
                pl.semaphore_wait(barrier, 2 * late)
                signal(go.at[1], partner)

            @pl.when(core == 0)
            def _():
                pl.semaphore_wait(go.at[1], 1)

            for link, edge in (("zp", late_p), ("zm", late_m)):

                @pl.when(edge > 0)
                def _():
                    for r in range(4):
                        send_along_z(link, r)

    def greet(i, who):
        for to in who:
            signal(ready.at[i], to)

    def met(i, who):
        pl.semaphore_wait(ready.at[i], len(who))

    def left_slot(i):
        origin = ((x - i // 4 + 4) % 4) * 4 + (y - i % 4 + 4) % 4
        return ((z - origin // 2 + 8) % 8) * 2 + (origin % 2 + core) % 2

    def right_slot(a):
        origin = ((z - a // 2 + 8) % 8) * 2 + (core + a % 2) % 2
        return ((x - origin // 4 + 4) % 4) * 4 + (y - origin % 4 + 4) % 4

    def pick(table, i):
        value = jnp.int32(table[0])
        for k in range(1, len(table)):
            if table[k] != table[0]:
                value = jnp.where(i == k, jnp.int32(table[k]), value)
        return value

    def multiply(a, i):
        acc[...] += jnp.dot(abuf[a], bbuf[i], preferred_element_type=jnp.float32)

    def event(e):
        todo = []
        for i in range(16):
            if EVENT_B[i] == e:
                a = left_slot(i)
                todo.append((a, jnp.int32(i), pick(EVENT_A, a) <= e))
        for a in range(16):
            if EVENT_A[a] == e:
                i = right_slot(a)
                todo.append((jnp.int32(a), i, pick(EVENT_B, i) < e))

        def step(t, carry):
            a, i, ok = todo[0]
            ok = ok.astype(jnp.int32)
            for k in range(1, len(todo)):
                a = jnp.where(t == k, todo[k][0], a)
                i = jnp.where(t == k, todo[k][1], i)
                ok = jnp.where(t == k, todo[k][2].astype(jnp.int32), ok)

            @pl.when(ok > 0)
            def _():
                multiply(a, i)

            return carry

        lax.fori_loop(0, len(todo), step, 0)

    def to_plane(src, dst, send, recv):
        for a in range(4):
            for b in range(4):
                if (a, b) != (0, 0):
                    copy = remote(src, dst.at[a * 4 + b], send.at[a * 4 + b], recv.at[a * 4 + b], at(a, b))
                    copy.start()
                    sent.append(copy)

    tiles.wait()
    mask(0)

    @pl.when(core == 0)
    def _():
        pl.semaphore_wait(barrier, 13 - 2 * late)
        signal(go.at[0], partner)

    @pl.when(core == 1)
    def _():
        pl.semaphore_wait(go.at[0], 1)

    for i in range(4):
        if i:
            mask(i)
        have.add((0, 0, i))
        advance()
        own_along_z(i)
        if i % 2:
            hand_over(0, i // 2)
    across(z != 0)
    greet(0, plane)
    acc[...] = jnp.zeros_like(acc)
    own_sum = jnp.zeros((1, BLK), jnp.float32)
    for i in range(4):
        own_sum = own_sum + jnp.sum(bbuf[0, pl.ds(i * TB, TB), :].astype(jnp.float32), axis=0, keepdims=True)
    pbuf[0] = own_sum
    for i in range(1, 3):
        met(i - 1, plane)
        greet(i, plane)
    met(2, plane)
    root = z * 2 + core
    slot = ((root // 4 - x + 4) % 4) * 4 + (root % 4 - y + 4) % 4
    is_root = slot == 0
    to_root = remote(pbuf.at[0], pbuf.at[slot], send_p, recv_p.at[slot], (root, col))

    @pl.when(slot != 0)
    def _():
        to_root.start()

    across(z == 0)
    greet(3, line)
    along_xy(0)
    along_xy(1)
    along_z("zm", 0)
    along_xy(2)
    along_z("zm", 1)
    along_z("zp", 0)
    met(3, line)
    greet(4, line)
    along_xy(3)
    along_z("zm", 2)
    along_z("zp", 1)
    take_over(0)
    event(0)

    @pl.when(is_root)
    def _():
        total = pbuf[0]
        for k in range(1, 16):
            arrived(pbuf.at[k], recv_p.at[k])
            total = total + pbuf[k]
        sbuf[0] = total

    for r in range(4, 15):
        along_xy(r)
        along_z("zm", r - 1)
        if r < 14:
            along_z("zp", r - 2)
        if r == 5:
            met(4, line)
            greet(5, line)
        if r == 7:
            met(5, line)
            for k in range(1, 16):
                copy = remote(sbuf.at[0], sbuf.at[1], send_s.at[k], recv_s, along(k // 2, k % 2))

                @pl.when(is_root)
                def _():
                    copy.start()

        if r in (7, 11, 14):
            for dz in {7: (1, 7), 11: (2, 6), 14: (3, 5)}[r]:
                take_over(dz)
        if r in (5, 7, 9, 11, 12, 13, 14):
            event(EVENT_OF_ROUND[r])
        if r == 11:
            @pl.when(slot != 0)
            def _():
                arrived(sbuf.at[1], recv_s)

            v = jnp.where(is_root, sbuf[0], sbuf[1])
            p0 = v.astype(jnp.bfloat16).astype(jnp.float32)
            p1 = (v - p0).astype(jnp.bfloat16).astype(jnp.float32)
            p2 = v - p0 - p1
            rows = lax.broadcasted_iota(jnp.int32, (16, BLK), 0)
            parts = jnp.where(rows == 0, p0, jnp.where(rows == 1, p1, jnp.where(rows == 2, p2, 0.0)))
            own = jnp.dot(parts.astype(jnp.bfloat16), bbuf[0], preferred_element_type=jnp.float32)
            vbuf[0] = jnp.sum(own, axis=0, keepdims=True)
            to_plane(vbuf.at[0], vbuf, send_v, recv_v)
    along_z("zp", 12)
    along_z("zp", 13)
    event(8)
    for fetch in rest:
        fetch.wait()
    col_means = vbuf[0]
    for k in range(1, 16):
        arrived(vbuf.at[k], recv_v.at[k])
        col_means = col_means + vbuf[k]
    cut = 0.125 * thr_ref[...].astype(jnp.float32) * (col_means / (BLK * 16))
    take_over(4)
    event(9)

    for j in range(4):
        total = jnp.zeros((1, TB), jnp.float32)
        for i in range(4):
            part = acc[pl.ds(i * TB, TB), pl.ds(j * TB, TB)]
            part = jnp.maximum(part - cut[:, j * TB : (j + 1) * TB], 0.0) * keep_ref[i, j].astype(jnp.float32)
            acc[pl.ds(i * TB, TB), pl.ds(j * TB, TB)] = part
            total = total + jnp.sum(part, axis=0, keepdims=True)
        tbuf[0, :, pl.ds(j * TB, TB)] = total
    to_plane(tbuf.at[0], tbuf, send_t, recv_t)
    for copy in sent:
        copy.wait_send()
    for link in ("zp", "zm"):
        for r in range(14):
            if (link, r) != ("zp", 13):
                z_copy(link, LINKS[link][r], r if link == "zp" else 14 + r).wait_send()

    @pl.when(z != 7)
    def _():
        z_copy("zp", ZP[13], 13).wait_send()

    @pl.when(z == 1)
    def _():
        z_copy("zm", (5, 1), 28).wait_send()

    @pl.when(slot != 0)
    def _():
        to_root.wait_send()

    @pl.when(is_root)
    def _():
        for k in range(1, 16):
            remote(sbuf.at[0], sbuf.at[1], send_s.at[k], recv_s, along(k // 2, k % 2)).wait_send()

    total = tbuf[0]
    for k in range(1, 16):
        arrived(tbuf.at[k], recv_t.at[k])
        total = total + tbuf[k]
    scale = 1.0 / jnp.maximum(total / (BLK * 16), 0.1)
    out_ref[...] = (acc[...] * scale).astype(jnp.bfloat16)


def on_device(values, tile_mask, keep_mask, thr_index):
    dma = pltpu.SemaphoreType.DMA
    return pl.pallas_call(
        kernel,
        out_shape=jax.ShapeDtypeStruct(values.shape, jnp.bfloat16),
        in_specs=[pl.BlockSpec(memory_space=pltpu.HBM)] * 4,
        out_specs=pl.BlockSpec(memory_space=pltpu.VMEM),
        scratch_shapes=[
            pltpu.VMEM((BLK, BLK), jnp.bfloat16),
            pltpu.SMEM((4, 4), jnp.int32),
            pltpu.SMEM((4, 4), jnp.int32),
            pltpu.VMEM((1, BLK), jnp.int32),
            pltpu.VMEM((16, BLK, BLK), jnp.bfloat16),
            pltpu.VMEM((16, BLK, BLK), jnp.bfloat16),
            pltpu.VMEM((BLK, BLK), jnp.float32),
            pltpu.VMEM((16, 1, BLK), jnp.float32),
            pltpu.VMEM((2, 1, BLK), jnp.float32),
            pltpu.VMEM((16, 1, BLK), jnp.float32),
            pltpu.VMEM((16, 1, BLK), jnp.float32),
            dma((7,)),
            dma((60,)),
            dma((29,)),
            dma((16,)),
            dma,
            dma((16,)),
            dma((16,)),
            dma((16,)),
            dma((16, 4)),
            dma((8, 4)),
            dma((8, 2)),
            dma((16,)),
            dma,
            dma((16,)),
            dma((16,)),
            pltpu.SemaphoreType.REGULAR((2,)),
            pltpu.SemaphoreType.REGULAR((6,)),
        ],
        compiler_params=pltpu.CompilerParams(collective_id=0, has_side_effects=True, vmem_limit_bytes=48 << 20),
    )(*[pltpu.with_memory_space_constraint(v, pltpu.HBM) for v in (values, tile_mask, keep_mask, thr_index.reshape(1, BLK))])


def solution(mesh):
    placed = (P("row", "col"), P("row", "col"), P("row", "col"), P("col"))
    return jax.shard_map(on_device, mesh=mesh, in_specs=placed, out_specs=P("row", "col"), check_vma=False)
```

```python
import jax
import jax.numpy as jnp
from jax import lax
from jax.experimental import pallas as pl
from jax.experimental.pallas import tpu as pltpu
from jax.sharding import PartitionSpec as P

TB = 128
BLK = 512
QR = 128
NX = 4
NZ = 8
MESH = pl.DeviceIdType.MESH

OWN = [(0, 0, 0, 2), (0, 0, 2, 2)]
XP = OWN + [(1, 0, 0, 1), (1, 0, 2, 1), (0, 1, 2, 2), (0, 3, 2, 2), (0, 2, 2, 2), (1, 1, 2, 1), (1, 3, 2, 1), (1, 2, 2, 1)]
XM = OWN + [((-dx) % 4, dy, q ^ (n % 2), n) for dx, dy, q, n in XP[2:]]
YP = OWN + [(dy, dx, q ^ 2, n) for dx, dy, q, n in [XP[3], XP[2]] + XP[4:]]
YM = OWN + [(dy, dx, q ^ 2, n) for dx, dy, q, n in [XM[3], XM[2]] + XM[4:]]
ZP = [(d, h) for d in (0, 1, 2) for h in (0, 1)] + [(3, 0)]
ZM = [(d, h) for d in (0, 7, 6) for h in (0, 1)] + [(5, 1)]
LINKS = {"xp": XP, "xm": XM, "yp": YP, "ym": YM, "zp": ZP, "zm": ZM}
BELOW = 176
STEP = {"xp": (1, 0), "xm": (3, 0), "yp": (0, 1), "ym": (0, 3), "zp": (1,), "zm": (7,)}


def land(link, piece):
    extent = 8 if link[0] == "z" else 4
    step = STEP[link]
    return tuple((a + b) % extent for a, b in zip(piece, step)) + piece[len(step) :]


EVENT_OF_ROUND = [0, 0, 0, 0, 1, 2, 3, 4, 5, 6]
EVENT_B = [0] * 16
for _link in ("xp", "xm", "yp", "ym"):
    for _r, _c in enumerate(LINKS[_link]):
        _l = land(_link, _c)
        EVENT_B[_l[0] * 4 + _l[1]] = max(EVENT_B[_l[0] * 4 + _l[1]], EVENT_OF_ROUND[_r])
EVENT_A = [0, 0, 0, 1, 2, 3, 5, 6, 6, 7, 3, 4, 1, 2, 0, 0]


def kernel(values_ref, tile_hbm, keep_hbm, thr_hbm, out_ref, raw, tile_ref, keep_ref, thr_ref, abuf, bbuf, acc, pbuf, sbuf,
           vbuf, tbuf, raw_sem, send_xy, send_z, send_d, send_p, send_s, send_v, send_t, recv_b, recv_a, recv_x, recv_d,
           recv_p, recv_s, recv_v, recv_t, go, ready):
    row, col = lax.axis_index("row"), lax.axis_index("col")
    x, y, z, core = row // 4, row % 4, col // 2, col % 2

    def at(dx, dy):
        return (((x + dx + 4) % 4) * 4 + (y + dy + 4) % 4, col)

    def along(dz, other):
        return (row, ((z + dz + 8) % 8) * 2 + (core + other) % 2)

    def signal(sem, to):
        pl.semaphore_signal(sem, inc=1, device_id=to, device_id_type=MESH)

    peer = {"xp": at(1, 0), "xm": at(-1, 0), "yp": at(0, 1), "ym": at(0, -1), "zp": along(1, 0), "zm": along(-1, 0)}
    partner = along(0, 1)
    plane = [peer[link] for link in ("xp", "xm", "yp", "ym")]
    line = [peer["zp"], peer["zm"]]
    late_p = z % 2
    late_m = 1 - z % 2

    barrier = pltpu.get_barrier_semaphore()
    for to in plane:
        signal(barrier, (to[0], z * 2))
    signal(barrier, (row, ((z + 1) % 8) * 2 + late_p))
    signal(barrier, (row, ((z + 7) % 8) * 2 + late_m))
    signal(barrier, partner)

    tiles = pltpu.make_async_copy(tile_hbm, tile_ref, raw_sem.at[0])
    tiles.start()
    fetches = [
        pltpu.make_async_copy(
            values_ref.at[pl.ds(i * QR, QR), :], raw.at[pl.ds(i * QR, QR), :], raw_sem.at[1 + i]
        )
        for i in range(4)
    ]
    for fetch in fetches:
        fetch.start()
    rest = [
        pltpu.make_async_copy(keep_hbm, keep_ref, raw_sem.at[5]),
        pltpu.make_async_copy(thr_hbm, thr_ref, raw_sem.at[6]),
    ]
    for fetch in rest:
        fetch.start()

    def mask(i):
        fetches[i].wait()
        for j in range(4):
            tile = raw[pl.ds(i * TB, TB), pl.ds(j * TB, TB)].astype(jnp.float32) * tile_ref[i, j].astype(jnp.float32)
            tile = tile.astype(jnp.bfloat16)
            abuf[0, pl.ds(i * TB, TB), pl.ds(j * TB, TB)] = tile
            bbuf[0, pl.ds(i * TB, TB), pl.ds(j * TB, TB)] = tile

    sent = []

    def remote(src, dst, ss, rs, to):
        return pltpu.make_async_remote_copy(src, dst, ss, rs, device_id=to, device_id_type=MESH)

    def arrived(ref, sem):
        remote(ref, ref, send_d.at[0], sem, partner).wait_recv()

    def rows_of(slot, q, n):
        return bbuf.at[slot, pl.ds(q * QR, n * QR), :]

    def half(slot, h):
        return abuf.at[slot, pl.ds(h * 256, 256), :]

    have = set()
    nxt = dict.fromkeys(("xp", "xm", "yp", "ym"), 0)
    n_xy = [0]

    def advance():
        more = True
        while more:
            more = False
            for link in nxt:
                if nxt[link] == len(LINKS[link]):
                    continue
                c = LINKS[link][nxt[link]]
                if any((c[0], c[1], c[2] + k) not in have for k in range(c[3])):
                    continue
                to = land(link, c)
                copy = remote(
                    rows_of(c[0] * 4 + c[1], c[2], c[3]),
                    rows_of(to[0] * 4 + to[1], to[2], to[3]),
                    send_xy.at[n_xy[0]],
                    recv_b.at[to[0] * 4 + to[1], to[2]],
                    peer[link],
                )
                copy.start()
                sent.append(copy)
                n_xy[0] += 1
                nxt[link] += 1
                more = True

    def along_xy(r):
        for link in nxt:
            to = land(link, LINKS[link][r])
            arrived(rows_of(to[0] * 4 + to[1], to[2], to[3]), recv_b.at[to[0] * 4 + to[1], to[2]])
            have.update((to[0], to[1], to[2] + k) for k in range(to[3]))
            advance()

    def z_copy(link, r):
        c = LINKS[link][r]
        to = land(link, c)
        return remote(
            half(c[0] * 2, c[1]),
            half(to[0] * 2, to[1]),
            send_z.at[r if link == "zp" else 7 + r],
            recv_a.at[to[0], to[1]],
            peer[link],
        )

    def z_part(link, source, start, size, slot, sem):
        rows = pl.ds(start, size)
        return remote(abuf.at[source * 2, rows, :], abuf.at[8, rows, :], send_z.at[slot], sem, peer[link])

    rest_rows = 256 - BELOW
    parts_p = [z_part("zp", 3, 0, BELOW, 6, recv_a.at[4, 0]), z_part("zp", 3, BELOW, rest_rows, 14, recv_x)]
    part_m = z_part("zm", 5, BELOW, rest_rows, 15, recv_x)

    def send_along_z(link, r):
        z_copy(link, r).start()

    def handed(dz, h):
        return remote(half(dz * 2, h), half(dz * 2 + 1, h), send_d.at[dz * 2 + h], recv_d.at[dz, h], partner)

    def hand_over(dz, h):
        handed(dz, h).start()

    def take_over(dz):
        for h in range(2):
            arrived(half(dz * 2 + 1, h), recv_d.at[dz, h])

    def along_z(link, r, when=None):
        if when is not None:
            pl.when(when)(lambda: along_z(link, r))
            return
        to = land(link, LINKS[link][r])
        if to == (4, 0):
            arrived(abuf.at[8, pl.ds(0, BELOW), :], recv_a.at[4, 0])
            arrived(abuf.at[8, pl.ds(BELOW, rest_rows), :], recv_x)
        else:
            arrived(half(to[0] * 2, to[1]), recv_a.at[to[0], to[1]])
        if (link, to) == ("zp", (3, 0)):
            parts_p[0].start()

            @pl.when(z != 7)
            def _():
                parts_p[1].start()

        elif to in LINKS[link]:
            send_along_z(link, LINKS[link].index(to))
        elif (link, to) == ("zm", (5, 0)):

            @pl.when(z == 1)
            def _():
                part_m.start()

        hand_over(*to)

    def own_along_z(q):
        @pl.when(late_p == 0)
        def _():
            send_along_z("zp", q)

        @pl.when(late_m == 0)
        def _():
            send_along_z("zm", q)

    def across(when):
        @pl.when(when)
        def _():
            @pl.when(core == 1)
            def _():
                pl.semaphore_wait(barrier, 3)
                signal(go.at[1], partner)

            @pl.when(core == 0)
            def _():
                pl.semaphore_wait(go.at[1], 1)

            for link, edge in (("zp", late_p), ("zm", late_m)):

                @pl.when(edge > 0)
                def _():
                    for h in range(2):
                        send_along_z(link, h)

    def greet(i, who):
        for to in who:
            signal(ready.at[i], to)

    def met(i, who):
        pl.semaphore_wait(ready.at[i], len(who))

    def left_slot(i):
        origin = ((x - i // 4 + 4) % 4) * 4 + (y - i % 4 + 4) % 4
        return ((z - origin // 2 + 8) % 8) * 2 + (origin % 2 + core) % 2

    def right_slot(a):
        origin = ((z - a // 2 + 8) % 8) * 2 + (core + a % 2) % 2
        return ((x - origin // 4 + 4) % 4) * 4 + (y - origin % 4 + 4) % 4

    def pick(table, i):
        value = jnp.int32(table[0])
        for k in range(1, len(table)):
            if table[k] != table[0]:
                value = jnp.where(i == k, jnp.int32(table[k]), value)
        return value

    def multiply(a, i):
        acc[...] += jnp.dot(abuf[a], bbuf[i], preferred_element_type=jnp.float32)

    def event(e):
        todo = []
        for i in range(16):
            if EVENT_B[i] == e:
                a = left_slot(i)
                todo.append((a, jnp.int32(i), pick(EVENT_A, a) <= e))
        for a in range(16):
            if EVENT_A[a] == e:
                i = right_slot(a)
                todo.append((jnp.int32(a), i, pick(EVENT_B, i) < e))

        def step(t, carry):
            a, i, ok = todo[0]
            ok = ok.astype(jnp.int32)
            for k in range(1, len(todo)):
                a = jnp.where(t == k, todo[k][0], a)
                i = jnp.where(t == k, todo[k][1], i)
                ok = jnp.where(t == k, todo[k][2].astype(jnp.int32), ok)

            @pl.when(ok > 0)
            def _():
                multiply(a, i)

            return carry

        lax.fori_loop(0, len(todo), step, 0)

    def to_plane(src, dst, send, recv):
        for a in (2, 1, 3, 0):
            for b in (2, 1, 3, 0):
                if (a, b) != (0, 0):
                    copy = remote(src, dst.at[a * 4 + b], send.at[a * 4 + b], recv.at[a * 4 + b], at(a, b))
                    copy.start()
                    sent.append(copy)

    tiles.wait()
    mask(0)

    @pl.when(z == 7)
    def _():
        for i in range(1, 4):
            mask(i)

    across(z == 7)

    @pl.when(core == 0)
    def _():
        pl.semaphore_wait(barrier, 11)
        signal(go.at[0], partner)

    @pl.when(core == 1)
    def _():
        pl.semaphore_wait(go.at[0], 1)

    for i in range(4):
        if i:

            @pl.when(z != 7)
            def _():
                mask(i)

        have.add((0, 0, i))
        if i % 2:
            advance()
            own_along_z(i // 2)
            hand_over(0, i // 2)
    across((z != 0) & (z != 7))
    greet(0, plane)
    acc[...] = jnp.zeros_like(acc)
    own_sum = jnp.zeros((1, BLK), jnp.float32)
    for i in range(4):
        own_sum = own_sum + jnp.sum(bbuf[0, pl.ds(i * TB, TB), :].astype(jnp.float32), axis=0, keepdims=True)
    pbuf[0] = own_sum
    for i in range(1, 3):
        met(i - 1, plane)
        greet(i, plane)
    met(2, plane)
    root = z * 2 + core
    slot = ((root // 4 - x + 4) % 4) * 4 + (root % 4 - y + 4) % 4
    is_root = slot == 0
    to_root = remote(pbuf.at[0], pbuf.at[slot], send_p, recv_p.at[slot], (root, col))

    @pl.when(slot != 0)
    def _():
        to_root.start()

    across(z == 0)
    greet(3, line)
    along_xy(0)
    along_z("zm", 0)
    along_z("zp", 0, z != 0)
    met(3, line)
    greet(4, line)
    along_xy(1)
    along_z("zm", 1)
    along_z("zp", 0, z == 0)
    along_z("zp", 1, z != 0)
    along_xy(2)

    @pl.when(is_root)
    def _():
        total = pbuf[0]
        for k in range(1, 16):
            arrived(pbuf.at[k], recv_p.at[k])
            total = total + pbuf[k]
        sbuf[0] = total

    for r in range(3, 10):
        if r == 9:
            along_z("zm", 6)
            along_z("zp", 6)
            take_over(3)
        along_xy(r)
        if r in (3, 4, 5, 6):
            along_z("zm", r - 1)
            along_z("zp", r - 2, z == 0)
            along_z("zp", r - 1, z != 0)
        if r == 8:
            along_z("zp", 5, z == 0)
        if r == 3:
            met(4, line)
            greet(5, line)
        if r == 4:
            met(5, line)
            for k in range(1, 16):
                copy = remote(sbuf.at[0], sbuf.at[1], send_s.at[k], recv_s, along(k // 2, k % 2))

                @pl.when(is_root)
                def _():
                    copy.start()

        for dz in {3: (0, 7), 4: (1,), 5: (6,), 6: (2,), 7: (5,)}.get(r, ()):
            take_over(dz)
        event(EVENT_OF_ROUND[r])
        if r == 6:
            @pl.when(slot != 0)
            def _():
                arrived(sbuf.at[1], recv_s)

            v = jnp.where(is_root, sbuf[0], sbuf[1])
            p0 = v.astype(jnp.bfloat16).astype(jnp.float32)
            p1 = (v - p0).astype(jnp.bfloat16).astype(jnp.float32)
            p2 = v - p0 - p1
            rows = lax.broadcasted_iota(jnp.int32, (16, BLK), 0)
            parts = jnp.where(rows == 0, p0, jnp.where(rows == 1, p1, jnp.where(rows == 2, p2, 0.0)))
            own = jnp.dot(parts.astype(jnp.bfloat16), bbuf[0], preferred_element_type=jnp.float32)
            vbuf[0] = jnp.sum(own, axis=0, keepdims=True)
            to_plane(vbuf.at[0], vbuf, send_v, recv_v)
    for fetch in rest:
        fetch.wait()
    col_means = vbuf[0]
    for k in range(1, 16):
        arrived(vbuf.at[k], recv_v.at[k])
        col_means = col_means + vbuf[k]
    cut = 0.125 * thr_ref[...].astype(jnp.float32) * (col_means / (BLK * 16))
    take_over(4)
    event(7)

    for j in range(4):
        total = jnp.zeros((1, TB), jnp.float32)
        for i in range(4):
            part = acc[pl.ds(i * TB, TB), pl.ds(j * TB, TB)]
            part = jnp.maximum(part - cut[:, j * TB : (j + 1) * TB], 0.0) * keep_ref[i, j].astype(jnp.float32)
            acc[pl.ds(i * TB, TB), pl.ds(j * TB, TB)] = part
            total = total + jnp.sum(part, axis=0, keepdims=True)
        tbuf[0, :, pl.ds(j * TB, TB)] = total
    to_plane(tbuf.at[0], tbuf, send_t, recv_t)
    for copy in sent:
        copy.wait_send()
    for dz in range(8):
        for h in range(2):
            handed(dz, h).wait_send()
    for link in ("zp", "zm"):
        for r in range(7):
            if (link, r) != ("zp", 6):
                z_copy(link, r).wait_send()
    parts_p[0].wait_send()

    @pl.when(z != 7)
    def _():
        parts_p[1].wait_send()

    @pl.when(z == 1)
    def _():
        part_m.wait_send()

    @pl.when(slot != 0)
    def _():
        to_root.wait_send()

    @pl.when(is_root)
    def _():
        for k in range(1, 16):
            remote(sbuf.at[0], sbuf.at[1], send_s.at[k], recv_s, along(k // 2, k % 2)).wait_send()

    total = tbuf[0]
    for k in range(1, 16):
        arrived(tbuf.at[k], recv_t.at[k])
        total = total + tbuf[k]
    scale = 1.0 / jnp.maximum(total / (BLK * 16), 0.1)
    out_ref[...] = (acc[...] * scale).astype(jnp.bfloat16)


def on_device(values, tile_mask, keep_mask, thr_index):
    dma = pltpu.SemaphoreType.DMA
    return pl.pallas_call(
        kernel,
        out_shape=jax.ShapeDtypeStruct(values.shape, jnp.bfloat16),
        in_specs=[pl.BlockSpec(memory_space=pltpu.HBM)] * 4,
        out_specs=pl.BlockSpec(memory_space=pltpu.VMEM),
        scratch_shapes=[
            pltpu.VMEM((BLK, BLK), jnp.bfloat16),
            pltpu.SMEM((4, 4), jnp.int32),
            pltpu.SMEM((4, 4), jnp.int32),
            pltpu.VMEM((1, BLK), jnp.int32),
            pltpu.VMEM((16, BLK, BLK), jnp.bfloat16),
            pltpu.VMEM((16, BLK, BLK), jnp.bfloat16),
            pltpu.VMEM((BLK, BLK), jnp.float32),
            pltpu.VMEM((16, 1, BLK), jnp.float32),
            pltpu.VMEM((2, 1, BLK), jnp.float32),
            pltpu.VMEM((16, 1, BLK), jnp.float32),
            pltpu.VMEM((16, 1, BLK), jnp.float32),
            dma((7,)),
            dma((40,)),
            dma((16,)),
            dma((16,)),
            dma,
            dma((16,)),
            dma((16,)),
            dma((16,)),
            dma((16, 4)),
            dma((8, 2)),
            dma,
            dma((8, 2)),
            dma((16,)),
            dma,
            dma((16,)),
            dma((16,)),
            pltpu.SemaphoreType.REGULAR((2,)),
            pltpu.SemaphoreType.REGULAR((6,)),
        ],
        compiler_params=pltpu.CompilerParams(collective_id=0, has_side_effects=True, vmem_limit_bytes=48 << 20),
    )(*[pltpu.with_memory_space_constraint(v, pltpu.HBM) for v in (values, tile_mask, keep_mask, thr_index.reshape(1, BLK))])


def solution(mesh):
    placed = (P("row", "col"), P("row", "col"), P("row", "col"), P("col"))
    return jax.shard_map(on_device, mesh=mesh, in_specs=placed, out_specs=P("row", "col"), check_vma=False)
```

```python
import jax
import jax.numpy as jnp
from jax import lax
from jax.experimental import pallas as pl
from jax.experimental.pallas import tpu as pltpu
from jax.sharding import PartitionSpec as P

TB = 128
BLK = 512
QR = 128
NX = 4
NZ = 8
MESH = pl.DeviceIdType.MESH

UP, DOWN = [(0, 0, 0, 2), (0, 0, 2, 2)], [(0, 0, 2, 2), (0, 0, 0, 2)]
XP = UP + [(1, 0, 0, 2), (0, 1, 2, 2), (0, 3, 2, 2), (0, 2, 2, 2), (1, 1, 2, 1), (1, 3, 2, 1), (1, 2, 2, 1)]
XM = DOWN + [((-dx) % 4, dy, 2 if n == 2 else q ^ 1, n) for dx, dy, q, n in XP[2:]]
YP = UP + [(0, 1, 0, 2)] + [(dy, dx, q ^ 2, n) for dx, dy, q, n in XP[3:]]
YM = DOWN + [(0, 3, 2, 2)] + [(dy, dx, q ^ 2, n) for dx, dy, q, n in XM[3:]]
ZP = [(d, h) for d in (0, 1, 2) for h in (0, 1)] + [(3, 0)]
ZM = [(d, h) for d in (0, 7, 6) for h in (0, 1)] + [(5, 1)]
LINKS = {"xp": XP, "xm": XM, "yp": YP, "ym": YM, "zp": ZP, "zm": ZM}
BELOW = 128
STEP = {"xp": (1, 0), "xm": (3, 0), "yp": (0, 1), "ym": (0, 3), "zp": (1,), "zm": (7,)}


def land(link, piece):
    extent = 8 if link[0] == "z" else 4
    step = STEP[link]
    return tuple((a + b) % extent for a, b in zip(piece, step)) + piece[len(step) :]


EVENT_OF_ROUND = [0, 0, 0, 1, 2, 3, 4, 5, 7]
EVENT_B = [0] * 16
for _link in ("xp", "xm", "yp", "ym"):
    for _r, _c in enumerate(LINKS[_link]):
        _l = land(_link, _c)
        EVENT_B[_l[0] * 4 + _l[1]] = max(EVENT_B[_l[0] * 4 + _l[1]], EVENT_OF_ROUND[_r])
EVENT_A = [0, 0, 0, 1, 2, 3, 5, 6, 6, 8, 3, 4, 1, 2, 0, 0]


def kernel(values_ref, tile_hbm, keep_hbm, thr_hbm, out_ref, raw, tile_ref, keep_ref, thr_ref, abuf, bbuf, acc, pbuf, sbuf,
           vbuf, tbuf, raw_sem, send_xy, send_z, send_d, send_p, send_s, send_v, send_t, recv_b, recv_a, recv_x, recv_d,
           recv_p, recv_s, recv_v, recv_t, go, ready):
    row, col = lax.axis_index("row"), lax.axis_index("col")
    x, y, z, core = row // 4, row % 4, col // 2, col % 2

    def at(dx, dy):
        return (((x + dx + 4) % 4) * 4 + (y + dy + 4) % 4, col)

    def along(dz, other):
        return (row, ((z + dz + 8) % 8) * 2 + (core + other) % 2)

    def signal(sem, to):
        pl.semaphore_signal(sem, inc=1, device_id=to, device_id_type=MESH)

    peer = {"xp": at(1, 0), "xm": at(-1, 0), "yp": at(0, 1), "ym": at(0, -1), "zp": along(1, 0), "zm": along(-1, 0)}
    partner = along(0, 1)
    plane = [peer[link] for link in ("xp", "xm", "yp", "ym")]
    line = [peer["zp"], peer["zm"]]
    late_p = z % 2
    late_m = 1 - z % 2

    lead = 1 - z // 7
    above, below = (z + 1) % 8, (z + 7) % 8
    barrier = pltpu.get_barrier_semaphore()
    for to in plane:
        signal(barrier, (to[0], z * 2 + lead))
    signal(barrier, (row, above * 2 + (late_p + 1 - above // 7) % 2))
    signal(barrier, (row, below * 2 + (late_m + 1 - below // 7) % 2))
    signal(barrier, partner)

    tiles = pltpu.make_async_copy(tile_hbm, tile_ref, raw_sem.at[0])
    tiles.start()
    fetches = [
        pltpu.make_async_copy(
            values_ref.at[pl.ds(i * QR, QR), :], raw.at[pl.ds(i * QR, QR), :], raw_sem.at[1 + i]
        )
        for i in range(4)
    ]
    for fetch in fetches:
        fetch.start()
    rest = [
        pltpu.make_async_copy(keep_hbm, keep_ref, raw_sem.at[5]),
        pltpu.make_async_copy(thr_hbm, thr_ref, raw_sem.at[6]),
    ]
    for fetch in rest:
        fetch.start()

    def mask(i):
        fetches[i].wait()
        for j in range(4):
            tile = raw[pl.ds(i * TB, TB), pl.ds(j * TB, TB)].astype(jnp.float32) * tile_ref[i, j].astype(jnp.float32)
            tile = tile.astype(jnp.bfloat16)
            abuf[0, pl.ds(i * TB, TB), pl.ds(j * TB, TB)] = tile
            bbuf[0, pl.ds(i * TB, TB), pl.ds(j * TB, TB)] = tile

    sent = []

    def remote(src, dst, ss, rs, to):
        return pltpu.make_async_remote_copy(src, dst, ss, rs, device_id=to, device_id_type=MESH)

    def arrived(ref, sem):
        remote(ref, ref, send_d.at[0], sem, partner).wait_recv()

    def rows_of(slot, q, n):
        return bbuf.at[slot, pl.ds(q * QR, n * QR), :]

    def half(slot, h):
        return abuf.at[slot, pl.ds(h * 256, 256), :]

    have = set()
    nxt = dict.fromkeys(("xp", "xm", "yp", "ym"), 0)
    n_xy = [0]

    def advance():
        more = True
        while more:
            more = False
            for link in nxt:
                if nxt[link] == len(LINKS[link]):
                    continue
                c = LINKS[link][nxt[link]]
                if any((c[0], c[1], c[2] + k) not in have for k in range(c[3])):
                    continue
                to = land(link, c)
                copy = remote(
                    rows_of(c[0] * 4 + c[1], c[2], c[3]),
                    rows_of(to[0] * 4 + to[1], to[2], to[3]),
                    send_xy.at[n_xy[0]],
                    recv_b.at[to[0] * 4 + to[1], to[2]],
                    peer[link],
                )
                copy.start()
                sent.append(copy)
                n_xy[0] += 1
                nxt[link] += 1
                more = True

    def along_xy(r):
        for link in nxt:
            to = land(link, LINKS[link][r])
            arrived(rows_of(to[0] * 4 + to[1], to[2], to[3]), recv_b.at[to[0] * 4 + to[1], to[2]])
            have.update((to[0], to[1], to[2] + k) for k in range(to[3]))
            advance()

    def z_copy(link, r):
        c = LINKS[link][r]
        to = land(link, c)
        return remote(
            half(c[0] * 2, c[1]),
            half(to[0] * 2, to[1]),
            send_z.at[r if link == "zp" else 7 + r],
            recv_a.at[to[0], to[1]],
            peer[link],
        )

    def z_part(link, source, start, size, slot, sem):
        rows = pl.ds(start, size)
        return remote(abuf.at[source * 2, rows, :], abuf.at[8, rows, :], send_z.at[slot], sem, peer[link])

    rest_rows = 256 - BELOW
    parts_p = [z_part("zp", 3, 0, BELOW, 6, recv_a.at[4, 0]), z_part("zp", 3, BELOW, rest_rows, 14, recv_x)]
    part_m = z_part("zm", 5, BELOW, rest_rows, 15, recv_x)

    def send_along_z(link, r):
        z_copy(link, r).start()

    def handed(dz, h):
        return remote(half(dz * 2, h), half(dz * 2 + 1, h), send_d.at[dz * 2 + h], recv_d.at[dz, h], partner)

    def hand_over(dz, h):
        handed(dz, h).start()

    def take_over(dz):
        for h in range(2):
            arrived(half(dz * 2 + 1, h), recv_d.at[dz, h])

    def along_z(link, r, when=None):
        if when is not None:
            pl.when(when)(lambda: along_z(link, r))
            return
        to = land(link, LINKS[link][r])
        if to == (4, 0):
            arrived(abuf.at[8, pl.ds(0, BELOW), :], recv_a.at[4, 0])
            arrived(abuf.at[8, pl.ds(BELOW, rest_rows), :], recv_x)
        else:
            arrived(half(to[0] * 2, to[1]), recv_a.at[to[0], to[1]])
        if (link, to) == ("zp", (3, 0)):
            parts_p[0].start()

            @pl.when(z != 7)
            def _():
                parts_p[1].start()

        elif to in LINKS[link]:
            send_along_z(link, LINKS[link].index(to))
        elif (link, to) == ("zm", (5, 0)):

            @pl.when(z == 1)
            def _():
                part_m.start()

        hand_over(*to)

    def own_along_z(q):
        @pl.when(late_p == 0)
        def _():
            send_along_z("zp", q)

        @pl.when(late_m == 0)
        def _():
            send_along_z("zm", q)

    def meet(when):
        @pl.when(when & (core != lead))
        def _():
            pl.semaphore_wait(barrier, 3)
            signal(go.at[1], partner)

    def across(when):
        @pl.when(when)
        def _():
            @pl.when(core == lead)
            def _():
                pl.semaphore_wait(go.at[1], 1)

            for link, edge in (("zp", late_p), ("zm", late_m)):

                @pl.when(edge > 0)
                def _():
                    for h in range(2):
                        send_along_z(link, h)

    def greet(i, who):
        for to in who:
            signal(ready.at[i], to)

    def met(i, who):
        pl.semaphore_wait(ready.at[i], len(who))

    def left_slot(i):
        origin = ((x - i // 4 + 4) % 4) * 4 + (y - i % 4 + 4) % 4
        return ((z - origin // 2 + 8) % 8) * 2 + (origin % 2 + core) % 2

    def right_slot(a):
        origin = ((z - a // 2 + 8) % 8) * 2 + (core + a % 2) % 2
        return ((x - origin // 4 + 4) % 4) * 4 + (y - origin % 4 + 4) % 4

    def pick(table, i):
        value = jnp.int32(table[0])
        for k in range(1, len(table)):
            if table[k] != table[0]:
                value = jnp.where(i == k, jnp.int32(table[k]), value)
        return value

    def multiply(a, i):
        acc[...] += jnp.dot(abuf[a], bbuf[i], preferred_element_type=jnp.float32)

    def event(e):
        todo = []
        for i in range(16):
            if EVENT_B[i] == e:
                a = left_slot(i)
                todo.append((a, jnp.int32(i), pick(EVENT_A, a) <= e))
        for a in range(16):
            if EVENT_A[a] == e:
                i = right_slot(a)
                todo.append((jnp.int32(a), i, pick(EVENT_B, i) < e))

        def step(t, carry):
            a, i, ok = todo[0]
            ok = ok.astype(jnp.int32)
            for k in range(1, len(todo)):
                a = jnp.where(t == k, todo[k][0], a)
                i = jnp.where(t == k, todo[k][1], i)
                ok = jnp.where(t == k, todo[k][2].astype(jnp.int32), ok)

            @pl.when(ok > 0)
            def _():
                multiply(a, i)

            return carry

        lax.fori_loop(0, len(todo), step, 0)

    def to_plane(src, dst, send, recv):
        for a in (2, 1, 3, 0):
            for b in (2, 1, 3, 0):
                if (a, b) != (0, 0):
                    copy = remote(src, dst.at[a * 4 + b], send.at[a * 4 + b], recv.at[a * 4 + b], at(a, b))
                    copy.start()
                    sent.append(copy)

    tiles.wait()
    mask(0)

    @pl.when(z == 7)
    def _():
        for i in range(1, 4):
            mask(i)

    meet(z == 7)
    across(z == 7)
    prompt = (z == 2) | ((z > 3) & (z < 7))
    meet(prompt)

    @pl.when(core == lead)
    def _():
        pl.semaphore_wait(barrier, 11)
        signal(go.at[0], partner)

    @pl.when(core != lead)
    def _():
        pl.semaphore_wait(go.at[0], 1)

    for i in range(4):
        if i:

            @pl.when(z != 7)
            def _():
                mask(i)

        have.add((0, 0, i))
        if i % 2:
            advance()
            own_along_z(i // 2)
            hand_over(0, i // 2)
    meet((z == 1) | (z == 3))
    across((z != 0) & (z != 7))
    greet(0, plane)
    acc[...] = jnp.zeros_like(acc)
    own_sum = jnp.zeros((1, BLK), jnp.float32)
    for i in range(4):
        own_sum = own_sum + jnp.sum(bbuf[0, pl.ds(i * TB, TB), :].astype(jnp.float32), axis=0, keepdims=True)
    pbuf[0] = own_sum
    for i in range(1, 3):
        met(i - 1, plane)
        greet(i, plane)
    met(2, plane)
    root = z * 2 + core
    slot = ((root // 4 - x + 4) % 4) * 4 + (root % 4 - y + 4) % 4
    is_root = slot == 0
    to_root = remote(pbuf.at[0], pbuf.at[slot], send_p, recv_p.at[slot], (root, col))

    @pl.when(slot != 0)
    def _():
        to_root.start()

    meet(z == 0)
    across(z == 0)
    greet(3, line)
    along_xy(0)
    along_z("zm", 0)
    along_z("zp", 0, z != 0)
    met(3, line)
    greet(4, line)
    along_xy(1)
    along_z("zm", 1)
    along_z("zp", 0, z == 0)
    along_z("zp", 1, z != 0)

    @pl.when(is_root)
    def _():
        total = pbuf[0]
        for k in range(1, 16):
            arrived(pbuf.at[k], recv_p.at[k])
            total = total + pbuf[k]
        sbuf[0] = total

    for r in range(2, 9):
        if r == 8:
            along_z("zm", 6)
            along_z("zp", 6)
            take_over(3)
            event(6)
        along_xy(r)
        if r in (2, 3, 4, 5):
            along_z("zm", r)
            along_z("zp", r - 1, z == 0)
            along_z("zp", r, z != 0)
        if r == 7:
            along_z("zp", 5, z == 0)
        if r == 2:
            met(4, line)
            greet(5, line)
        if r == 3:
            met(5, line)
            for k in range(1, 16):
                copy = remote(sbuf.at[0], sbuf.at[1], send_s.at[k], recv_s, along(k // 2, k % 2))

                @pl.when(is_root)
                def _():
                    copy.start()

        for dz in {2: (0, 7), 3: (1,), 4: (6,), 5: (2,), 6: (5,)}.get(r, ()):
            take_over(dz)
        event(EVENT_OF_ROUND[r])
        if r == 5:
            @pl.when(slot != 0)
            def _():
                arrived(sbuf.at[1], recv_s)

            v = jnp.where(is_root, sbuf[0], sbuf[1])
            p0 = v.astype(jnp.bfloat16).astype(jnp.float32)
            p1 = (v - p0).astype(jnp.bfloat16).astype(jnp.float32)
            p2 = v - p0 - p1
            rows = lax.broadcasted_iota(jnp.int32, (16, BLK), 0)
            parts = jnp.where(rows == 0, p0, jnp.where(rows == 1, p1, jnp.where(rows == 2, p2, 0.0)))
            own = jnp.dot(parts.astype(jnp.bfloat16), bbuf[0], preferred_element_type=jnp.float32)
            vbuf[0] = jnp.sum(own, axis=0, keepdims=True)
            to_plane(vbuf.at[0], vbuf, send_v, recv_v)
    for fetch in rest:
        fetch.wait()
    col_means = vbuf[0]
    for k in range(1, 16):
        arrived(vbuf.at[k], recv_v.at[k])
        col_means = col_means + vbuf[k]
    cut = 0.125 * thr_ref[...].astype(jnp.float32) * (col_means / (BLK * 16))
    take_over(4)
    event(8)

    for j in range(4):
        total = jnp.zeros((1, TB), jnp.float32)
        for i in range(4):
            part = acc[pl.ds(i * TB, TB), pl.ds(j * TB, TB)]
            part = jnp.maximum(part - cut[:, j * TB : (j + 1) * TB], 0.0) * keep_ref[i, j].astype(jnp.float32)
            acc[pl.ds(i * TB, TB), pl.ds(j * TB, TB)] = part
            total = total + jnp.sum(part, axis=0, keepdims=True)
        tbuf[0, :, pl.ds(j * TB, TB)] = total
    to_plane(tbuf.at[0], tbuf, send_t, recv_t)
    for copy in sent:
        copy.wait_send()
    for dz in range(8):
        for h in range(2):
            handed(dz, h).wait_send()
    for link in ("zp", "zm"):
        for r in range(7):
            if (link, r) != ("zp", 6):
                z_copy(link, r).wait_send()
    parts_p[0].wait_send()

    @pl.when(z != 7)
    def _():
        parts_p[1].wait_send()

    @pl.when(z == 1)
    def _():
        part_m.wait_send()

    @pl.when(slot != 0)
    def _():
        to_root.wait_send()

    @pl.when(is_root)
    def _():
        for k in range(1, 16):
            remote(sbuf.at[0], sbuf.at[1], send_s.at[k], recv_s, along(k // 2, k % 2)).wait_send()

    total = tbuf[0]
    for k in range(1, 16):
        arrived(tbuf.at[k], recv_t.at[k])
        total = total + tbuf[k]
    scale = 1.0 / jnp.maximum(total / (BLK * 16), 0.1)
    out_ref[...] = (acc[...] * scale).astype(jnp.bfloat16)


def on_device(values, tile_mask, keep_mask, thr_index):
    dma = pltpu.SemaphoreType.DMA
    return pl.pallas_call(
        kernel,
        out_shape=jax.ShapeDtypeStruct(values.shape, jnp.bfloat16),
        in_specs=[pl.BlockSpec(memory_space=pltpu.HBM)] * 4,
        out_specs=pl.BlockSpec(memory_space=pltpu.VMEM),
        scratch_shapes=[
            pltpu.VMEM((BLK, BLK), jnp.bfloat16),
            pltpu.SMEM((4, 4), jnp.int32),
            pltpu.SMEM((4, 4), jnp.int32),
            pltpu.VMEM((1, BLK), jnp.int32),
            pltpu.VMEM((16, BLK, BLK), jnp.bfloat16),
            pltpu.VMEM((16, BLK, BLK), jnp.bfloat16),
            pltpu.VMEM((BLK, BLK), jnp.float32),
            pltpu.VMEM((16, 1, BLK), jnp.float32),
            pltpu.VMEM((2, 1, BLK), jnp.float32),
            pltpu.VMEM((16, 1, BLK), jnp.float32),
            pltpu.VMEM((16, 1, BLK), jnp.float32),
            dma((7,)),
            dma((40,)),
            dma((16,)),
            dma((16,)),
            dma,
            dma((16,)),
            dma((16,)),
            dma((16,)),
            dma((16, 4)),
            dma((8, 2)),
            dma,
            dma((8, 2)),
            dma((16,)),
            dma,
            dma((16,)),
            dma((16,)),
            pltpu.SemaphoreType.REGULAR((2,)),
            pltpu.SemaphoreType.REGULAR((6,)),
        ],
        compiler_params=pltpu.CompilerParams(collective_id=0, has_side_effects=True, vmem_limit_bytes=48 << 20),
    )(*[pltpu.with_memory_space_constraint(v, pltpu.HBM) for v in (values, tile_mask, keep_mask, thr_index.reshape(1, BLK))])


def solution(mesh):
    placed = (P("row", "col"), P("row", "col"), P("row", "col"), P("col"))
    return jax.shard_map(on_device, mesh=mesh, in_specs=placed, out_specs=P("row", "col"), check_vma=False)
```

```python
import jax
import jax.numpy as jnp
from jax import lax
from jax.experimental import pallas as pl
from jax.experimental.pallas import tpu as pltpu
from jax.sharding import PartitionSpec as P

TB = 128
BLK = 512
QR = 128
NX = 4
NZ = 8
MESH = pl.DeviceIdType.MESH

UP, DOWN = [(0, 0, 0, 2), (0, 0, 2, 2)], [(0, 0, 2, 2), (0, 0, 0, 2)]
XP = UP + [(1, 0, 0, 2), (0, 1, 2, 2), (0, 3, 2, 2), (0, 2, 2, 2), (1, 1, 2, 1), (1, 3, 2, 1), (1, 2, 2, 1)]
XM = DOWN + [((-dx) % 4, dy, 2 if n == 2 else q ^ 1, n) for dx, dy, q, n in XP[2:]]
YP = UP + [(0, 1, 0, 2)] + [(dy, dx, q ^ 2, n) for dx, dy, q, n in XP[3:]]
YM = DOWN + [(0, 3, 2, 2)] + [(dy, dx, q ^ 2, n) for dx, dy, q, n in XM[3:]]
ZP = [(d, h) for d in (0, 1, 2) for h in (0, 1)] + [(3, 0)]
ZM = [(d, h) for d in (0, 7, 6) for h in (0, 1)] + [(5, 1)]
LINKS = {"xp": XP, "xm": XM, "yp": YP, "ym": YM, "zp": ZP, "zm": ZM}
BELOW = 128
STEP = {"xp": (1, 0), "xm": (3, 0), "yp": (0, 1), "ym": (0, 3), "zp": (1,), "zm": (7,)}


def land(link, piece):
    extent = 8 if link[0] == "z" else 4
    step = STEP[link]
    return tuple((a + b) % extent for a, b in zip(piece, step)) + piece[len(step) :]


EVENT_OF_ROUND = [0, 0, 0, 1, 2, 3, 4, 5, 7]
EVENT_B = [0] * 16
for _link in ("xp", "xm", "yp", "ym"):
    for _r, _c in enumerate(LINKS[_link]):
        _l = land(_link, _c)
        EVENT_B[_l[0] * 4 + _l[1]] = max(EVENT_B[_l[0] * 4 + _l[1]], EVENT_OF_ROUND[_r])
EVENT_A = [0, 0, 0, 1, 2, 3, 5, 6, 6, 8, 3, 4, 1, 2, 0, 0]


def kernel(values_ref, tile_hbm, keep_hbm, thr_hbm, out_ref, raw, tile_ref, keep_ref, thr_ref, abuf, bbuf, acc, pbuf, sbuf,
           vbuf, tbuf, raw_sem, send_xy, send_z, send_d, send_p, send_s, send_v, send_t, recv_b, recv_a, recv_x, recv_d,
           recv_p, recv_s, recv_v, recv_t, go, ready):
    row, col = lax.axis_index("row"), lax.axis_index("col")
    x, y, z, core = row // 4, row % 4, col // 2, col % 2

    def at(dx, dy):
        return (((x + dx + 4) % 4) * 4 + (y + dy + 4) % 4, col)

    def along(dz, other):
        return (row, ((z + dz + 8) % 8) * 2 + (core + other) % 2)

    def signal(sem, to):
        pl.semaphore_signal(sem, inc=1, device_id=to, device_id_type=MESH)

    peer = {"xp": at(1, 0), "xm": at(-1, 0), "yp": at(0, 1), "ym": at(0, -1), "zp": along(1, 0), "zm": along(-1, 0)}
    partner = along(0, 1)
    plane = [peer[link] for link in ("xp", "xm", "yp", "ym")]
    line = [peer["zp"], peer["zm"]]
    late_p = z % 2
    late_m = 1 - z % 2

    lead = 1 - z // 7
    above, below = (z + 1) % 8, (z + 7) % 8
    barrier = pltpu.get_barrier_semaphore()
    for to in plane:
        signal(barrier, (to[0], z * 2 + lead))
    signal(barrier, (row, above * 2 + (late_p + 1 - above // 7) % 2))
    signal(barrier, (row, below * 2 + (late_m + 1 - below // 7) % 2))
    signal(barrier, partner)

    tiles = pltpu.make_async_copy(tile_hbm, tile_ref, raw_sem.at[0])
    tiles.start()
    fetches = [
        pltpu.make_async_copy(
            values_ref.at[pl.ds(i * QR, QR), :], raw.at[pl.ds(i * QR, QR), :], raw_sem.at[1 + i]
        )
        for i in range(4)
    ]
    for fetch in fetches:
        fetch.start()
    rest = [
        pltpu.make_async_copy(keep_hbm, keep_ref, raw_sem.at[5]),
        pltpu.make_async_copy(thr_hbm, thr_ref, raw_sem.at[6]),
    ]
    for fetch in rest:
        fetch.start()

    def mask(i):
        fetches[i].wait()
        for j in range(4):
            tile = raw[pl.ds(i * TB, TB), pl.ds(j * TB, TB)].astype(jnp.float32) * tile_ref[i, j].astype(jnp.float32)
            tile = tile.astype(jnp.bfloat16)
            abuf[0, pl.ds(i * TB, TB), pl.ds(j * TB, TB)] = tile
            bbuf[0, pl.ds(i * TB, TB), pl.ds(j * TB, TB)] = tile

    sent = []

    def remote(src, dst, ss, rs, to):
        return pltpu.make_async_remote_copy(src, dst, ss, rs, device_id=to, device_id_type=MESH)

    def arrived(ref, sem):
        remote(ref, ref, send_d.at[0], sem, partner).wait_recv()

    def rows_of(slot, q, n):
        return bbuf.at[slot, pl.ds(q * QR, n * QR), :]

    def half(slot, h):
        return abuf.at[slot, pl.ds(h * 256, 256), :]

    have = set()
    nxt = dict.fromkeys(("xp", "xm", "yp", "ym"), 0)
    n_xy = [0]

    def advance():
        more = True
        while more:
            more = False
            for link in nxt:
                if nxt[link] == len(LINKS[link]):
                    continue
                c = LINKS[link][nxt[link]]
                if any((c[0], c[1], c[2] + k) not in have for k in range(c[3])):
                    continue
                to = land(link, c)
                copy = remote(
                    rows_of(c[0] * 4 + c[1], c[2], c[3]),
                    rows_of(to[0] * 4 + to[1], to[2], to[3]),
                    send_xy.at[n_xy[0]],
                    recv_b.at[to[0] * 4 + to[1], to[2]],
                    peer[link],
                )
                copy.start()
                sent.append(copy)
                n_xy[0] += 1
                nxt[link] += 1
                more = True

    def along_xy(r):
        for link in nxt:
            to = land(link, LINKS[link][r])
            arrived(rows_of(to[0] * 4 + to[1], to[2], to[3]), recv_b.at[to[0] * 4 + to[1], to[2]])
            have.update((to[0], to[1], to[2] + k) for k in range(to[3]))
            advance()

    def z_copy(link, r):
        c = LINKS[link][r]
        to = land(link, c)
        return remote(
            half(c[0] * 2, c[1]),
            half(to[0] * 2, to[1]),
            send_z.at[r if link == "zp" else 7 + r],
            recv_a.at[to[0], to[1]],
            peer[link],
        )

    def z_part(link, source, start, size, slot, sem):
        rows = pl.ds(start, size)
        return remote(abuf.at[source * 2, rows, :], abuf.at[8, rows, :], send_z.at[slot], sem, peer[link])

    rest_rows = 256 - BELOW
    parts_p = [z_part("zp", 3, 0, BELOW, 6, recv_a.at[4, 0]), z_part("zp", 3, BELOW, rest_rows, 14, recv_x)]
    part_m = z_part("zm", 5, BELOW, rest_rows, 15, recv_x)

    def send_along_z(link, r):
        z_copy(link, r).start()

    def handed(dz, h):
        return remote(half(dz * 2, h), half(dz * 2 + 1, h), send_d.at[dz * 2 + h], recv_d.at[dz, h], partner)

    def hand_over(dz, h):
        handed(dz, h).start()

    def take_over(dz):
        for h in range(2):
            arrived(half(dz * 2 + 1, h), recv_d.at[dz, h])

    def along_z(link, r, when=None):
        if when is not None:
            pl.when(when)(lambda: along_z(link, r))
            return
        to = land(link, LINKS[link][r])
        if to == (4, 0):
            arrived(abuf.at[8, pl.ds(0, BELOW), :], recv_a.at[4, 0])
            arrived(abuf.at[8, pl.ds(BELOW, rest_rows), :], recv_x)
        else:
            arrived(half(to[0] * 2, to[1]), recv_a.at[to[0], to[1]])
        if (link, to) == ("zp", (3, 0)):
            parts_p[0].start()

            @pl.when(z != 7)
            def _():
                parts_p[1].start()

        elif to in LINKS[link]:
            send_along_z(link, LINKS[link].index(to))
        elif (link, to) == ("zm", (5, 0)):

            @pl.when(z == 1)
            def _():
                part_m.start()

        hand_over(*to)

    def own_along_z(q):
        @pl.when(late_p == 0)
        def _():
            send_along_z("zp", q)

        @pl.when(late_m == 0)
        def _():
            send_along_z("zm", q)

    def meet(when):
        @pl.when(when & (core != lead))
        def _():
            pl.semaphore_wait(barrier, 3)
            signal(go.at[1], partner)

    def across(when):
        @pl.when(when)
        def _():
            @pl.when(core == lead)
            def _():
                pl.semaphore_wait(go.at[1], 1)

            for link, edge in (("zp", late_p), ("zm", late_m)):

                @pl.when(edge > 0)
                def _():
                    for h in range(2):
                        send_along_z(link, h)

    def greet(i, who):
        for to in who:
            signal(ready.at[i], to)

    def met(i, who):
        pl.semaphore_wait(ready.at[i], len(who))

    def left_slot(i):
        origin = ((x - i // 4 + 4) % 4) * 4 + (y - i % 4 + 4) % 4
        return ((z - origin // 2 + 8) % 8) * 2 + (origin % 2 + core) % 2

    def right_slot(a):
        origin = ((z - a // 2 + 8) % 8) * 2 + (core + a % 2) % 2
        return ((x - origin // 4 + 4) % 4) * 4 + (y - origin % 4 + 4) % 4

    def pick(table, i):
        value = jnp.int32(table[0])
        for k in range(1, len(table)):
            if table[k] != table[0]:
                value = jnp.where(i == k, jnp.int32(table[k]), value)
        return value

    def multiply(a, i):
        acc[...] += jnp.dot(abuf[a], bbuf[i], preferred_element_type=jnp.float32)

    def event(e):
        todo = []
        for i in range(16):
            if EVENT_B[i] == e:
                a = left_slot(i)
                todo.append((a, jnp.int32(i), pick(EVENT_A, a) <= e))
        for a in range(16):
            if EVENT_A[a] == e:
                i = right_slot(a)
                todo.append((jnp.int32(a), i, pick(EVENT_B, i) < e))

        def step(t, carry):
            a, i, ok = todo[0]
            ok = ok.astype(jnp.int32)
            for k in range(1, len(todo)):
                a = jnp.where(t == k, todo[k][0], a)
                i = jnp.where(t == k, todo[k][1], i)
                ok = jnp.where(t == k, todo[k][2].astype(jnp.int32), ok)

            @pl.when(ok > 0)
            def _():
                multiply(a, i)

            return carry

        lax.fori_loop(0, len(todo), step, 0)

    def to_plane(src, dst, send, recv):
        for a in (2, 1, 3, 0):
            for b in (2, 1, 3, 0):
                if (a, b) != (0, 0):
                    copy = remote(src, dst.at[a * 4 + b], send.at[a * 4 + b], recv.at[a * 4 + b], at(a, b))
                    copy.start()
                    sent.append(copy)

    tiles.wait()
    mask(0)

    @pl.when(z == 7)
    def _():
        for i in range(1, 4):
            mask(i)

    meet(z == 7)
    across(z == 7)
    prompt = (z == 2) | ((z > 3) & (z < 7))
    meet(prompt)

    @pl.when(core == lead)
    def _():
        pl.semaphore_wait(barrier, 11)
        signal(go.at[0], partner)

    @pl.when(core != lead)
    def _():
        pl.semaphore_wait(go.at[0], 1)

    for i in range(4):
        if i:

            @pl.when(z != 7)
            def _():
                mask(i)

        have.add((0, 0, i))
        if i % 2:
            advance()
            own_along_z(i // 2)
            hand_over(0, i // 2)
    meet((z == 1) | (z == 3))
    across((z != 0) & (z != 7))
    greet(0, plane)
    acc[...] = jnp.zeros_like(acc)
    own_sum = jnp.zeros((1, BLK), jnp.float32)
    for i in range(4):
        own_sum = own_sum + jnp.sum(bbuf[0, pl.ds(i * TB, TB), :].astype(jnp.float32), axis=0, keepdims=True)
    pbuf[0] = own_sum
    for i in range(1, 3):
        met(i - 1, plane)
        greet(i, plane)
    met(2, plane)
    root = z * 2 + core
    slot = ((root // 4 - x + 4) % 4) * 4 + (root % 4 - y + 4) % 4
    is_root = slot == 0
    to_root = remote(pbuf.at[0], pbuf.at[slot], send_p, recv_p.at[slot], (root, col))

    @pl.when(slot != 0)
    def _():
        to_root.start()

    meet(z == 0)
    across(z == 0)
    greet(3, line)
    along_xy(0)
    along_z("zm", 0)
    along_z("zp", 0, z != 0)
    met(3, line)
    greet(4, line)
    along_xy(1)
    along_z("zm", 1)
    along_z("zp", 0, z == 0)
    along_z("zp", 1, z != 0)

    @pl.when(is_root)
    def _():
        total = pbuf[0]
        for k in range(1, 16):
            arrived(pbuf.at[k], recv_p.at[k])
            total = total + pbuf[k]
        sbuf[0] = total

    for r in range(2, 9):
        if r == 8:
            along_z("zm", 6)
            along_z("zp", 6)
            take_over(3)
            event(6)
        along_xy(r)
        if r in (2, 3, 4, 5):
            along_z("zm", r)
            along_z("zp", r - 1, z == 0)
            along_z("zp", r, z != 0)
        if r == 7:
            along_z("zp", 5, z == 0)
        if r == 2:
            met(4, line)
            greet(5, line)
        if r == 3:
            met(5, line)
            for k in range(1, 16):
                copy = remote(sbuf.at[0], sbuf.at[1], send_s.at[k], recv_s, along(k // 2, k % 2))

                @pl.when(is_root)
                def _():
                    copy.start()

        for dz in {2: (0, 7), 3: (1,), 4: (6,), 5: (2,), 6: (5,)}.get(r, ()):
            take_over(dz)
        event(EVENT_OF_ROUND[r])
        if r == 6:
            @pl.when(slot != 0)
            def _():
                arrived(sbuf.at[1], recv_s)

            v = jnp.where(is_root, sbuf[0], sbuf[1])
            p0 = v.astype(jnp.bfloat16).astype(jnp.float32)
            p1 = (v - p0).astype(jnp.bfloat16).astype(jnp.float32)
            p2 = v - p0 - p1
            rows = lax.broadcasted_iota(jnp.int32, (16, BLK), 0)
            parts = jnp.where(rows == 0, p0, jnp.where(rows == 1, p1, jnp.where(rows == 2, p2, 0.0)))
            own = jnp.dot(parts.astype(jnp.bfloat16), bbuf[0], preferred_element_type=jnp.float32)
            vbuf[0] = jnp.sum(own, axis=0, keepdims=True)
            to_plane(vbuf.at[0], vbuf, send_v, recv_v)
    for fetch in rest:
        fetch.wait()
    col_means = vbuf[0]
    for k in range(1, 16):
        arrived(vbuf.at[k], recv_v.at[k])
        col_means = col_means + vbuf[k]
    cut = 0.125 * thr_ref[...].astype(jnp.float32) * (col_means / (BLK * 16))
    take_over(4)
    event(8)

    for j in range(4):
        total = jnp.zeros((1, TB), jnp.float32)
        for i in range(4):
            part = acc[pl.ds(i * TB, TB), pl.ds(j * TB, TB)]
            part = jnp.maximum(part - cut[:, j * TB : (j + 1) * TB], 0.0) * keep_ref[i, j].astype(jnp.float32)
            acc[pl.ds(i * TB, TB), pl.ds(j * TB, TB)] = part
            total = total + jnp.sum(part, axis=0, keepdims=True)
        tbuf[0, :, pl.ds(j * TB, TB)] = total
    to_plane(tbuf.at[0], tbuf, send_t, recv_t)
    for copy in sent:
        copy.wait_send()
    for dz in range(8):
        for h in range(2):
            handed(dz, h).wait_send()
    for link in ("zp", "zm"):
        for r in range(7):
            if (link, r) != ("zp", 6):
                z_copy(link, r).wait_send()
    parts_p[0].wait_send()

    @pl.when(z != 7)
    def _():
        parts_p[1].wait_send()

    @pl.when(z == 1)
    def _():
        part_m.wait_send()

    @pl.when(slot != 0)
    def _():
        to_root.wait_send()

    @pl.when(is_root)
    def _():
        for k in range(1, 16):
            remote(sbuf.at[0], sbuf.at[1], send_s.at[k], recv_s, along(k // 2, k % 2)).wait_send()

    total = tbuf[0]
    for k in range(1, 16):
        arrived(tbuf.at[k], recv_t.at[k])
        total = total + tbuf[k]
    scale = 1.0 / jnp.maximum(total / (BLK * 16), 0.1)
    out_ref[...] = (acc[...] * scale).astype(jnp.bfloat16)


def on_device(values, tile_mask, keep_mask, thr_index):
    dma = pltpu.SemaphoreType.DMA
    return pl.pallas_call(
        kernel,
        out_shape=jax.ShapeDtypeStruct(values.shape, jnp.bfloat16),
        in_specs=[pl.BlockSpec(memory_space=pltpu.HBM)] * 4,
        out_specs=pl.BlockSpec(memory_space=pltpu.VMEM),
        scratch_shapes=[
            pltpu.VMEM((BLK, BLK), jnp.bfloat16),
            pltpu.SMEM((4, 4), jnp.int32),
            pltpu.SMEM((4, 4), jnp.int32),
            pltpu.VMEM((1, BLK), jnp.int32),
            pltpu.VMEM((16, BLK, BLK), jnp.bfloat16),
            pltpu.VMEM((16, BLK, BLK), jnp.bfloat16),
            pltpu.VMEM((BLK, BLK), jnp.float32),
            pltpu.VMEM((16, 1, BLK), jnp.float32),
            pltpu.VMEM((2, 1, BLK), jnp.float32),
            pltpu.VMEM((16, 1, BLK), jnp.float32),
            pltpu.VMEM((16, 1, BLK), jnp.float32),
            dma((7,)),
            dma((40,)),
            dma((16,)),
            dma((16,)),
            dma,
            dma((16,)),
            dma((16,)),
            dma((16,)),
            dma((16, 4)),
            dma((8, 2)),
            dma,
            dma((8, 2)),
            dma((16,)),
            dma,
            dma((16,)),
            dma((16,)),
            pltpu.SemaphoreType.REGULAR((2,)),
            pltpu.SemaphoreType.REGULAR((6,)),
        ],
        compiler_params=pltpu.CompilerParams(collective_id=0, has_side_effects=True, vmem_limit_bytes=48 << 20),
    )(*[pltpu.with_memory_space_constraint(v, pltpu.HBM) for v in (values, tile_mask, keep_mask, thr_index.reshape(1, BLK))])


def solution(mesh):
    placed = (P("row", "col"), P("row", "col"), P("row", "col"), P("col"))
    return jax.shard_map(on_device, mesh=mesh, in_specs=placed, out_specs=P("row", "col"), check_vma=False)
```

```python
import jax
import jax.numpy as jnp
from jax import lax
from jax.experimental import pallas as pl
from jax.experimental.pallas import tpu as pltpu
from jax.sharding import PartitionSpec as P

TB = 128
BLK = 512
QR = 128
NX = 4
NZ = 8
MESH = pl.DeviceIdType.MESH

UP, DOWN = [(0, 0, 0, 2), (0, 0, 2, 2)], [(0, 0, 2, 2), (0, 0, 0, 2)]
XP = UP + [(1, 0, 0, 2), (0, 1, 2, 2), (0, 3, 2, 2), (0, 2, 2, 2), (1, 1, 2, 1), (1, 3, 2, 1), (1, 2, 2, 1)]
XM = DOWN + [((-dx) % 4, dy, 2 if n == 2 else q ^ 1, n) for dx, dy, q, n in XP[2:]]
YP = UP + [(0, 1, 0, 2)] + [(dy, dx, q ^ 2, n) for dx, dy, q, n in XP[3:]]
YM = DOWN + [(0, 3, 2, 2)] + [(dy, dx, q ^ 2, n) for dx, dy, q, n in XM[3:]]
ZP = [(d, h) for d in (0, 1, 2) for h in (0, 1)] + [(3, 0)]
ZM = [(d, h) for d in (0, 7, 6) for h in (0, 1)] + [(5, 1)]
LINKS = {"xp": XP, "xm": XM, "yp": YP, "ym": YM, "zp": ZP, "zm": ZM}
BELOW = 160
STEP = {"xp": (1, 0), "xm": (3, 0), "yp": (0, 1), "ym": (0, 3), "zp": (1,), "zm": (7,)}


def land(link, piece):
    extent = 8 if link[0] == "z" else 4
    step = STEP[link]
    return tuple((a + b) % extent for a, b in zip(piece, step)) + piece[len(step) :]


EVENT_OF_ROUND = [0, 0, 0, 1, 2, 3, 4, 5, 7]
EVENT_B = [0] * 16
for _link in ("xp", "xm", "yp", "ym"):
    for _r, _c in enumerate(LINKS[_link]):
        _l = land(_link, _c)
        EVENT_B[_l[0] * 4 + _l[1]] = max(EVENT_B[_l[0] * 4 + _l[1]], EVENT_OF_ROUND[_r])
EVENT_A = [0, 0, 0, 1, 2, 3, 5, 6, 6, 8, 3, 4, 1, 2, 0, 0]


def kernel(values_ref, tile_hbm, keep_hbm, thr_hbm, out_ref, raw, tile_ref, keep_ref, thr_ref, abuf, bbuf, acc, pbuf, sbuf,
           vbuf, tbuf, raw_sem, send_xy, send_z, send_d, send_p, send_s, send_v, send_t, recv_b, recv_a, recv_x, recv_d,
           recv_p, recv_s, recv_v, recv_t, go, ready):
    row, col = lax.axis_index("row"), lax.axis_index("col")
    x, y, z, core = row // 4, row % 4, col // 2, col % 2

    def at(dx, dy):
        return (((x + dx + 4) % 4) * 4 + (y + dy + 4) % 4, col)

    def along(dz, other):
        return (row, ((z + dz + 8) % 8) * 2 + (core + other) % 2)

    def signal(sem, to):
        pl.semaphore_signal(sem, inc=1, device_id=to, device_id_type=MESH)

    peer = {"xp": at(1, 0), "xm": at(-1, 0), "yp": at(0, 1), "ym": at(0, -1), "zp": along(1, 0), "zm": along(-1, 0)}
    partner = along(0, 1)
    plane = [peer[link] for link in ("xp", "xm", "yp", "ym")]
    line = [peer["zp"], peer["zm"]]
    late_p = z % 2
    late_m = 1 - z % 2

    lead = 1 - z // 7
    above, below = (z + 1) % 8, (z + 7) % 8
    barrier = pltpu.get_barrier_semaphore()
    for to in plane:
        signal(barrier, (to[0], z * 2 + lead))
    signal(barrier, (row, above * 2 + (late_p + 1 - above // 7) % 2))
    signal(barrier, (row, below * 2 + (late_m + 1 - below // 7) % 2))
    signal(barrier, partner)

    tiles = pltpu.make_async_copy(tile_hbm, tile_ref, raw_sem.at[0])
    tiles.start()
    fetches = [
        pltpu.make_async_copy(
            values_ref.at[pl.ds(i * QR, QR), :], raw.at[pl.ds(i * QR, QR), :], raw_sem.at[1 + i]
        )
        for i in range(4)
    ]
    for fetch in fetches:
        fetch.start()
    rest = [
        pltpu.make_async_copy(keep_hbm, keep_ref, raw_sem.at[5]),
        pltpu.make_async_copy(thr_hbm, thr_ref, raw_sem.at[6]),
    ]
    for fetch in rest:
        fetch.start()

    def mask(i):
        fetches[i].wait()
        for j in range(4):
            tile = raw[pl.ds(i * TB, TB), pl.ds(j * TB, TB)].astype(jnp.float32) * tile_ref[i, j].astype(jnp.float32)
            tile = tile.astype(jnp.bfloat16)
            abuf[0, pl.ds(i * TB, TB), pl.ds(j * TB, TB)] = tile
            bbuf[0, pl.ds(i * TB, TB), pl.ds(j * TB, TB)] = tile

    sent = []

    def remote(src, dst, ss, rs, to):
        return pltpu.make_async_remote_copy(src, dst, ss, rs, device_id=to, device_id_type=MESH)

    def arrived(ref, sem):
        remote(ref, ref, send_d.at[0], sem, partner).wait_recv()

    def rows_of(slot, q, n):
        return bbuf.at[slot, pl.ds(q * QR, n * QR), :]

    def half(slot, h):
        return abuf.at[slot, pl.ds(h * 256, 256), :]

    have = set()
    nxt = dict.fromkeys(("xp", "xm", "yp", "ym"), 0)
    n_xy = [0]

    def advance():
        more = True
        while more:
            more = False
            for link in nxt:
                if nxt[link] == len(LINKS[link]):
                    continue
                c = LINKS[link][nxt[link]]
                if any((c[0], c[1], c[2] + k) not in have for k in range(c[3])):
                    continue
                to = land(link, c)
                copy = remote(
                    rows_of(c[0] * 4 + c[1], c[2], c[3]),
                    rows_of(to[0] * 4 + to[1], to[2], to[3]),
                    send_xy.at[n_xy[0]],
                    recv_b.at[to[0] * 4 + to[1], to[2]],
                    peer[link],
                )
                copy.start()
                sent.append(copy)
                n_xy[0] += 1
                nxt[link] += 1
                more = True

    def along_xy(r):
        for link in nxt:
            to = land(link, LINKS[link][r])
            arrived(rows_of(to[0] * 4 + to[1], to[2], to[3]), recv_b.at[to[0] * 4 + to[1], to[2]])
            have.update((to[0], to[1], to[2] + k) for k in range(to[3]))
            advance()

    def z_copy(link, r):
        c = LINKS[link][r]
        to = land(link, c)
        return remote(
            half(c[0] * 2, c[1]),
            half(to[0] * 2, to[1]),
            send_z.at[r if link == "zp" else 7 + r],
            recv_a.at[to[0], to[1]],
            peer[link],
        )

    def z_part(link, source, start, size, slot, sem):
        rows = pl.ds(start, size)
        return remote(abuf.at[source * 2, rows, :], abuf.at[8, rows, :], send_z.at[slot], sem, peer[link])

    rest_rows = 256 - BELOW
    parts_p = [z_part("zp", 3, 0, BELOW, 6, recv_a.at[4, 0]), z_part("zp", 3, BELOW, rest_rows, 14, recv_x)]
    part_m = z_part("zm", 5, BELOW, rest_rows, 15, recv_x)

    def send_along_z(link, r):
        z_copy(link, r).start()

    def handed(dz, h):
        return remote(half(dz * 2, h), half(dz * 2 + 1, h), send_d.at[dz * 2 + h], recv_d.at[dz, h], partner)

    def hand_over(dz, h):
        handed(dz, h).start()

    def take_over(dz):
        for h in range(2):
            arrived(half(dz * 2 + 1, h), recv_d.at[dz, h])

    def along_z(link, r, when=None):
        if when is not None:
            pl.when(when)(lambda: along_z(link, r))
            return
        to = land(link, LINKS[link][r])
        if to == (4, 0):
            arrived(abuf.at[8, pl.ds(0, BELOW), :], recv_a.at[4, 0])
            arrived(abuf.at[8, pl.ds(BELOW, rest_rows), :], recv_x)
        else:
            arrived(half(to[0] * 2, to[1]), recv_a.at[to[0], to[1]])
        if (link, to) == ("zp", (3, 0)):
            parts_p[0].start()

            @pl.when(z != 7)
            def _():
                parts_p[1].start()

        elif to in LINKS[link]:
            send_along_z(link, LINKS[link].index(to))
        elif (link, to) == ("zm", (5, 0)):

            @pl.when(z == 1)
            def _():
                part_m.start()

        hand_over(*to)

    def own_along_z(q):
        @pl.when(late_p == 0)
        def _():
            send_along_z("zp", q)

        @pl.when(late_m == 0)
        def _():
            send_along_z("zm", q)

    def meet(when):
        @pl.when(when & (core != lead))
        def _():
            pl.semaphore_wait(barrier, 3)
            signal(go.at[1], partner)

    def across(when):
        @pl.when(when)
        def _():
            @pl.when(core == lead)
            def _():
                pl.semaphore_wait(go.at[1], 1)

            for link, edge in (("zp", late_p), ("zm", late_m)):

                @pl.when(edge > 0)
                def _():
                    for h in range(2):
                        send_along_z(link, h)

    def greet(i, who):
        for to in who:
            signal(ready.at[i], to)

    def met(i, who):
        pl.semaphore_wait(ready.at[i], len(who))

    def left_slot(i):
        origin = ((x - i // 4 + 4) % 4) * 4 + (y - i % 4 + 4) % 4
        return ((z - origin // 2 + 8) % 8) * 2 + (origin % 2 + core) % 2

    def right_slot(a):
        origin = ((z - a // 2 + 8) % 8) * 2 + (core + a % 2) % 2
        return ((x - origin // 4 + 4) % 4) * 4 + (y - origin % 4 + 4) % 4

    def pick(table, i):
        value = jnp.int32(table[0])
        for k in range(1, len(table)):
            if table[k] != table[0]:
                value = jnp.where(i == k, jnp.int32(table[k]), value)
        return value

    def multiply(a, i):
        acc[...] += jnp.dot(abuf[a], bbuf[i], preferred_element_type=jnp.float32)

    def event(e):
        todo = []
        for i in range(16):
            if EVENT_B[i] == e:
                a = left_slot(i)
                todo.append((a, jnp.int32(i), pick(EVENT_A, a) <= e))
        for a in range(16):
            if EVENT_A[a] == e:
                i = right_slot(a)
                todo.append((jnp.int32(a), i, pick(EVENT_B, i) < e))

        def step(t, carry):
            a, i, ok = todo[0]
            ok = ok.astype(jnp.int32)
            for k in range(1, len(todo)):
                a = jnp.where(t == k, todo[k][0], a)
                i = jnp.where(t == k, todo[k][1], i)
                ok = jnp.where(t == k, todo[k][2].astype(jnp.int32), ok)

            @pl.when(ok > 0)
            def _():
                multiply(a, i)

            return carry

        if len(todo) == 1:
            pl.when(todo[0][2])(lambda: multiply(*todo[0][:2]))
        else:
            lax.fori_loop(0, len(todo), step, 0)

    def to_plane(src, dst, send, recv):
        for a in (2, 1, 3, 0):
            for b in (2, 1, 3, 0):
                if (a, b) != (0, 0):
                    copy = remote(src, dst.at[a * 4 + b], send.at[a * 4 + b], recv.at[a * 4 + b], at(a, b))
                    copy.start()
                    sent.append(copy)

    tiles.wait()
    mask(0)

    @pl.when(z == 7)
    def _():
        for i in range(1, 4):
            mask(i)

    meet(z == 7)
    across(z == 7)
    prompt = (z == 2) | ((z > 3) & (z < 7))
    meet(prompt)

    @pl.when(core == lead)
    def _():
        pl.semaphore_wait(barrier, 11)
        signal(go.at[0], partner)

    @pl.when(core != lead)
    def _():
        pl.semaphore_wait(go.at[0], 1)

    for i in range(4):
        if i:

            @pl.when(z != 7)
            def _():
                mask(i)

        have.add((0, 0, i))
        if i % 2:
            advance()
            own_along_z(i // 2)
            hand_over(0, i // 2)
    meet((z == 1) | (z == 3))
    across((z != 0) & (z != 7))
    greet(0, plane)
    acc[...] = jnp.zeros_like(acc)
    own_sum = jnp.zeros((1, BLK), jnp.float32)
    for i in range(4):
        own_sum = own_sum + jnp.sum(bbuf[0, pl.ds(i * TB, TB), :].astype(jnp.float32), axis=0, keepdims=True)
    pbuf[0] = own_sum
    for i in range(1, 3):
        met(i - 1, plane)
        greet(i, plane)
    met(2, plane)
    root = z * 2 + core
    slot = ((root // 4 - x + 4) % 4) * 4 + (root % 4 - y + 4) % 4
    is_root = slot == 0
    to_root = remote(pbuf.at[0], pbuf.at[slot], send_p, recv_p.at[slot], (root, col))

    @pl.when(slot != 0)
    def _():
        to_root.start()

    meet(z == 0)
    across(z == 0)
    greet(3, line)
    along_xy(0)
    along_z("zm", 0)
    along_z("zp", 0, z != 0)
    met(3, line)
    greet(4, line)
    along_xy(1)
    along_z("zm", 1)
    along_z("zp", 0, z == 0)
    along_z("zp", 1, z != 0)

    @pl.when(is_root)
    def _():
        total = pbuf[0]
        for k in range(1, 16):
            arrived(pbuf.at[k], recv_p.at[k])
            total = total + pbuf[k]
        sbuf[0] = total

    for r in range(2, 9):
        if r == 8:
            along_z("zm", 6)
            along_z("zp", 6)
            take_over(3)
            event(6)
        along_xy(r)
        if r in (2, 3, 4, 5):
            along_z("zm", r)
            along_z("zp", r - 1, z == 0)
            along_z("zp", r, z != 0)
        if r == 7:
            along_z("zp", 5, z == 0)
        if r == 2:
            met(4, line)
            greet(5, line)
        if r == 3:
            met(5, line)
            for k in range(1, 16):
                copy = remote(sbuf.at[0], sbuf.at[1], send_s.at[k], recv_s, along(k // 2, k % 2))

                @pl.when(is_root)
                def _():
                    copy.start()

        for dz in {2: (0, 7), 3: (1,), 4: (6,), 5: (2,), 6: (5,)}.get(r, ()):
            take_over(dz)
        event(EVENT_OF_ROUND[r])
        if r == 6:
            @pl.when(slot != 0)
            def _():
                arrived(sbuf.at[1], recv_s)

            v = jnp.where(is_root, sbuf[0], sbuf[1])
            p0 = v.astype(jnp.bfloat16).astype(jnp.float32)
            p1 = (v - p0).astype(jnp.bfloat16).astype(jnp.float32)
            p2 = v - p0 - p1
            rows = lax.broadcasted_iota(jnp.int32, (16, BLK), 0)
            parts = jnp.where(rows == 0, p0, jnp.where(rows == 1, p1, jnp.where(rows == 2, p2, 0.0)))
            own = jnp.dot(parts.astype(jnp.bfloat16), bbuf[0], preferred_element_type=jnp.float32)
            vbuf[0] = jnp.sum(own, axis=0, keepdims=True)
            to_plane(vbuf.at[0], vbuf, send_v, recv_v)
    for fetch in rest:
        fetch.wait()
    col_means = vbuf[0]
    for k in range(1, 16):
        arrived(vbuf.at[k], recv_v.at[k])
        col_means = col_means + vbuf[k]
    cut = 0.125 * thr_ref[...].astype(jnp.float32) * (col_means / (BLK * 16))
    take_over(4)
    event(8)

    for j in range(4):
        total = jnp.zeros((1, TB), jnp.float32)
        for i in range(4):
            part = acc[pl.ds(i * TB, TB), pl.ds(j * TB, TB)]
            part = jnp.maximum(part - cut[:, j * TB : (j + 1) * TB], 0.0) * keep_ref[i, j].astype(jnp.float32)
            acc[pl.ds(i * TB, TB), pl.ds(j * TB, TB)] = part
            total = total + jnp.sum(part, axis=0, keepdims=True)
        tbuf[0, :, pl.ds(j * TB, TB)] = total
    to_plane(tbuf.at[0], tbuf, send_t, recv_t)
    for copy in sent:
        copy.wait_send()
    for dz in range(8):
        for h in range(2):
            handed(dz, h).wait_send()
    for link in ("zp", "zm"):
        for r in range(7):
            if (link, r) != ("zp", 6):
                z_copy(link, r).wait_send()
    parts_p[0].wait_send()

    @pl.when(z != 7)
    def _():
        parts_p[1].wait_send()

    @pl.when(z == 1)
    def _():
        part_m.wait_send()

    @pl.when(slot != 0)
    def _():
        to_root.wait_send()

    @pl.when(is_root)
    def _():
        for k in range(1, 16):
            remote(sbuf.at[0], sbuf.at[1], send_s.at[k], recv_s, along(k // 2, k % 2)).wait_send()

    total = tbuf[0]
    for k in range(1, 16):
        arrived(tbuf.at[k], recv_t.at[k])
        total = total + tbuf[k]
    scale = 1.0 / jnp.maximum(total / (BLK * 16), 0.1)
    out_ref[...] = (acc[...] * scale).astype(jnp.bfloat16)


def on_device(values, tile_mask, keep_mask, thr_index):
    dma = pltpu.SemaphoreType.DMA
    return pl.pallas_call(
        kernel,
        out_shape=jax.ShapeDtypeStruct(values.shape, jnp.bfloat16),
        in_specs=[pl.BlockSpec(memory_space=pltpu.HBM)] * 4,
        out_specs=pl.BlockSpec(memory_space=pltpu.VMEM),
        scratch_shapes=[
            pltpu.VMEM((BLK, BLK), jnp.bfloat16),
            pltpu.SMEM((4, 4), jnp.int32),
            pltpu.SMEM((4, 4), jnp.int32),
            pltpu.VMEM((1, BLK), jnp.int32),
            pltpu.VMEM((16, BLK, BLK), jnp.bfloat16),
            pltpu.VMEM((16, BLK, BLK), jnp.bfloat16),
            pltpu.VMEM((BLK, BLK), jnp.float32),
            pltpu.VMEM((16, 1, BLK), jnp.float32),
            pltpu.VMEM((2, 1, BLK), jnp.float32),
            pltpu.VMEM((16, 1, BLK), jnp.float32),
            pltpu.VMEM((16, 1, BLK), jnp.float32),
            dma((7,)),
            dma((40,)),
            dma((16,)),
            dma((16,)),
            dma,
            dma((16,)),
            dma((16,)),
            dma((16,)),
            dma((16, 4)),
            dma((8, 2)),
            dma,
            dma((8, 2)),
            dma((16,)),
            dma,
            dma((16,)),
            dma((16,)),
            pltpu.SemaphoreType.REGULAR((2,)),
            pltpu.SemaphoreType.REGULAR((6,)),
        ],
        compiler_params=pltpu.CompilerParams(collective_id=0, has_side_effects=True, vmem_limit_bytes=48 << 20),
    )(*[pltpu.with_memory_space_constraint(v, pltpu.HBM) for v in (values, tile_mask, keep_mask, thr_index.reshape(1, BLK))])


def solution(mesh):
    placed = (P("row", "col"), P("row", "col"), P("row", "col"), P("col"))
    return jax.shard_map(on_device, mesh=mesh, in_specs=placed, out_specs=P("row", "col"), check_vma=False)
```
